128 devices in a mesh: gx: 16 (over z, x), gy: 8 (over y, core).
Axes of the slice: x: 4, y: 4, z: 4, core: 2. Of those that a mesh axis runs over, the one named last changes fastest.
Arguments:
- vectors: float32 [2, 256, 256, 548], P(None, 'gx', 'gy'), may hold values from -6 to 6
- diffusivity: float32 [256, 256], P('gx', 'gy'), may hold values from 0.2 to 0.25
- vertical_factor: float32 [548, 548], replicated, may hold values from -4 to 4, as said below
- weight_first: float32 [548, 768], replicated, may hold values from -0.25 to 0.25
- bias_first: float32 [768], replicated, may hold values from -3 to 3
- weight_second: float32 [768, 768], replicated, may hold values from -0.21875 to 0.21875
- bias_second: float32 [768], replicated, may hold values from -3 to 3
- weight_out: float32 [768, 616], replicated, may hold values from -0.21875 to 0.21875
- error_inverse: float32 [616, 616], replicated, may hold values from -4 to 4, as said below
- observed_column: int32 [65536], P(('gx', 'gy')), may hold values from 0 to 65535, as said below
- owner_count: int32 [128], P(('gx', 'gy')), may hold values from 4 to 512
- observed_state: float32 [65536, 548], P(('gx', 'gy')), may hold values from -6 to 6
- channel_mask: int32 [128, 616], replicated, may hold values 0 or 1
Outputs:
- products: float32 [2, 256, 256, 548], P(None, 'gx', 'gy')
The draws below stay inside these ranges and needn't reach their ends.
Inputs may be any that keep to these rules, and one draw needn't show every extreme that they name: `observed_column`: tile (a, b) holds the cells i with i // 16 = a and j with j // 32 = b. Among the used slots of one owner at most 4 lie in any one tile, and some tile receives exactly 4 from every owner. Unused slots hold valid columns. `vertical_factor`: the identity plus a dense random part; well conditioned. `error_inverse`: symmetric positive definite with a dominant diagonal.
All inputs are finite; a program needn't handle non-finite values.
Results may differ from the reference program's by a relative error of at most 0.0003.
Values sent between devices are 32-bit elements; how exact they have to be, the bound alone decides.
A program may use at most 128 MiB of HBM per device.

```python
import jax
import jax.numpy as jnp
from jax import lax

LEVELS = 548
UNITS = 768
CHANNELS = 616
SWEEPS = 4
CX = 16
CY = 32
SLOTS = 512
NX = 256
NY = 256
BUCKET = 4
N_GY = 8
DEVICES = 128


def obs_layout(key):
    key_shift = jax.random.fold_in(key, 11)
    key_count = jax.random.fold_in(key, 12)
    key_full = jax.random.fold_in(key, 13)
    key_order = jax.random.fold_in(key, 14)
    key_cell = jax.random.fold_in(key, 15)
    key_owner = jax.random.fold_in(key, 16)
    key_often = jax.random.fold_in(key, 17)
    key_side = jax.random.fold_in(key, 18)
    key_along = jax.random.fold_in(key, 19)
    key_which = jax.random.fold_in(key, 20)
    owners = DEVICES
    shifts = jax.random.randint(key_shift, (owners, 1), 0, 3)
    owner_cap = jnp.right_shift(jnp.full((owners, 1), BUCKET, jnp.int32), shifts)
    counts = jax.random.randint(key_count, (owners, DEVICES), 0, owner_cap + 1)
    full_dest = jax.random.randint(key_full, (), 0, DEVICES)
    counts = jnp.where(jnp.arange(DEVICES)[None, :] == full_dest, BUCKET, counts)
    full_owner = jax.random.randint(key_owner, (), 0, owners)
    counts = jnp.where(jnp.arange(owners)[:, None] == full_owner, BUCKET, counts)
    position = jnp.arange(SLOTS, dtype=jnp.int32)
    within = position % BUCKET
    target = position // BUCKET
    active = (within[None, :] < counts[:, target]).astype(jnp.int32)
    randoms = jax.random.randint(key_order, (owners, SLOTS), 0, SLOTS)
    scores = (1 - active) * SLOTS * SLOTS + randoms * SLOTS + position[None, :]
    ordering = jnp.argsort(scores, axis=1, stable=True)
    target_sorted = jnp.take_along_axis(jnp.broadcast_to(target[None, :], (owners, SLOTS)), ordering, axis=1)
    spread_cell = jax.random.randint(key_cell, (owners, SLOTS), 0, CX * CY)
    favoured_side = jax.random.randint(key_side, (DEVICES, 4), 0, 4)
    favoured_along = jax.random.randint(key_along, (DEVICES, 4), 0, CX * CY)
    which = jax.random.randint(key_which, (owners, SLOTS), 0, 4)
    often = jax.random.randint(key_often, (owners, SLOTS), 0, 3) == 0
    side = favoured_side[target_sorted, which]
    along = favoured_along[target_sorted, which]
    along_row = along % CX
    along_col = along % CY
    side_row = jnp.where(side == 0, 3, jnp.where(side == 1, CX - 4, along_row))
    side_col = jnp.where(side == 2, 3, jnp.where(side == 3, CY - 4, along_col))
    local_cell = jnp.where(often, side_row * CY + side_col, spread_cell)
    tile_a = target_sorted // N_GY
    tile_b = target_sorted % N_GY
    grid_row = tile_a * CX + local_cell // CY
    grid_col = tile_b * CY + local_cell % CY
    column = grid_row * (CY * N_GY) + grid_col
    return (column.reshape(-1).astype(jnp.int32), jnp.sum(counts, axis=1).astype(jnp.int32))


def draw_observed_column(key, part):
    return obs_layout(key)[0]


def draw_owner_count(key, part):
    return obs_layout(key)[1]


def draw_vertical_factor(key, part):
    noise = jax.random.normal(jax.random.fold_in(key, 21), (LEVELS, LEVELS), jnp.float32)
    return jnp.eye(LEVELS, dtype=jnp.float32) + 0.6 * noise / jnp.sqrt(jnp.float32(LEVELS))


def draw_error_inverse(key, part):
    noise = jax.random.normal(jax.random.fold_in(key, 31), (CHANNELS, CHANNELS), jnp.float32)
    diagonal = jax.random.uniform(jax.random.fold_in(key, 32), (CHANNELS,), jnp.float32, 1.5, 3.0)
    symmetric = (noise + noise.T) * (0.5 / jnp.sqrt(2.0 * CHANNELS))
    return symmetric + jnp.diag(diagonal)


def touch_ends(drawn, key, least, high):
    longest = drawn.shape.index(max(drawn.shape))
    spots = []
    for shift in (0, 1):
        where = [jax.random.randint(jax.random.fold_in(key, axis), (), 0, length) for axis, length in enumerate(drawn.shape)]
        where[longest] = (where[longest] + shift) % drawn.shape[longest]
        spots.append(tuple(where))
    return drawn.at[spots[0]].set(least).at[spots[1]].set(high)


def shard_levels(own_key, dims, cuts, smallest, top_value):
    loudness, own = 1.0, jax.random.fold_in(own_key, 6)
    for dim, shards_of in cuts:
        heights = jnp.exp(jax.random.uniform(jax.random.fold_in(own, dim), (shards_of,), jnp.float32, smallest / len(cuts), top_value / len(cuts)))
        loudness = loudness * jnp.repeat(heights, dims[dim] // shards_of).reshape([-1 if axis == dim else 1 for axis in range(len(dims))])
    return loudness


def bell_draw(rng, extent, spread, reach, cuts=(), kind=jnp.bfloat16):
    level = shard_levels(rng, extent, cuts, -0.22, 0.18) if cuts else 1.0
    values = jax.random.normal(rng, extent, jnp.float32) * spread * level
    return jnp.minimum(jnp.maximum(values, -reach), reach).astype(kind)


def setup_inputs(seed: int = 0) -> dict:
    seeds = jax.random.split(jax.random.key(seed), 14)
    return {
        "vectors": bell_draw(seeds[0], (2, NX, NY, LEVELS), 1.0, 6.0, ((1, 16), (2, 8)), jnp.float32),
        "diffusivity": jnp.clip(0.2 + 0.049999997 * jax.random.uniform(seeds[1], (NX, NY), jnp.float32) ** shard_levels(seeds[1], (NX, NY), ((0, 16), (1, 8)), -0.2, 0.2), 0.2, 0.25),
        "vertical_factor": draw_vertical_factor(jax.random.fold_in(seeds[13], 71), 0),
        "weight_first": bell_draw(seeds[3], (LEVELS, UNITS), LEVELS ** -0.5, 0.25, (), jnp.float32),
        "bias_first": bell_draw(seeds[4], (UNITS,), 0.5, 3.0, (), jnp.float32),
        "weight_second": bell_draw(seeds[5], (UNITS, UNITS), UNITS ** -0.5, 0.21875, (), jnp.float32),
        "bias_second": bell_draw(seeds[6], (UNITS,), 0.5, 3.0, (), jnp.float32),
        "weight_out": bell_draw(seeds[7], (UNITS, CHANNELS), UNITS ** -0.5, 0.21875, (), jnp.float32),
        "error_inverse": draw_error_inverse(jax.random.fold_in(seeds[13], 71), 0),
        "observed_column": draw_observed_column(jax.random.fold_in(seeds[13], 71), 0),
        "owner_count": draw_owner_count(jax.random.fold_in(seeds[13], 71), 0),
        "observed_state": bell_draw(seeds[11], (DEVICES * SLOTS, LEVELS), 1.0, 6.0, ((0, 128),), jnp.float32),
        "channel_mask": touch_ends((jax.random.randint(seeds[12], (DEVICES, CHANNELS), 0, 4) < 3).astype(jnp.int32), jax.random.fold_in(seeds[12], 1), 0, 1),
    }


HIGH = lax.Precision.HIGHEST


def laplace(field):
    padded = jnp.pad(field, ((0, 0), (1, 1), (1, 1), (0, 0)))
    beside_all = padded[:, 2:, 1:-1] + padded[:, :-2, 1:-1] + padded[:, 1:-1, 2:] + padded[:, 1:-1, :-2]
    return beside_all - 4.0 * field


def network(profile, perturb, gate, weight_first, bias_first, weight_second, bias_second, weight_out, error_inverse):
    hidden_one = jnp.tanh(jnp.dot(profile, weight_first, precision=HIGH) + bias_first)
    hidden_two = jnp.tanh(jnp.dot(hidden_one, weight_second, precision=HIGH) + bias_second)
    slope_one = 1.0 - hidden_one * hidden_one
    slope_two = 1.0 - hidden_two * hidden_two
    tangent = jnp.einsum("vnk,kh->vnh", perturb, weight_first, precision=HIGH) * slope_one
    tangent = jnp.einsum("vnh,hg->vng", tangent, weight_second, precision=HIGH) * slope_two
    tangent = jnp.einsum("vng,gc->vnc", tangent, weight_out, precision=HIGH)
    weighted = gate * jnp.einsum("vnc,cd->vnd", gate * tangent, error_inverse, precision=HIGH)
    gradient = jnp.einsum("vnc,gc->vng", weighted, weight_out, precision=HIGH) * slope_two
    gradient = jnp.einsum("vng,hg->vnh", gradient, weight_second, precision=HIGH) * slope_one
    return jnp.einsum("vnh,kh->vnk", gradient, weight_first, precision=HIGH)


def reference(vectors, diffusivity, vertical_factor, weight_first, bias_first, weight_second, bias_second, weight_out, error_inverse, observed_column, owner_count, observed_state, channel_mask):
    shape = vectors.shape
    increment = jnp.dot(vectors.reshape(-1, LEVELS), vertical_factor.T, precision=HIGH).reshape(shape)
    coeff = diffusivity[None, :, :, None]
    for sweep in range(SWEEPS):
        increment = increment + coeff * laplace(increment)
    states = increment.reshape(2, NX * NY, LEVELS)

    def owner_work(packed):
        columns, used_count, profile, mask_row = packed
        in_use = (jnp.arange(SLOTS, dtype=jnp.int32) < used_count).astype(jnp.float32)
        gate = mask_row.astype(jnp.float32)[None, :] * in_use[:, None]
        perturb = states[:, columns]
        return network(profile, perturb, gate, weight_first, bias_first, weight_second, bias_second, weight_out, error_inverse)

    gradient = lax.map(owner_work, (observed_column.reshape(DEVICES, SLOTS), owner_count, observed_state.reshape(DEVICES, SLOTS, LEVELS), channel_mask))
    gradient = jnp.transpose(gradient, (1, 0, 2, 3)).reshape(2, DEVICES * SLOTS, LEVELS)
    field = jnp.zeros((2, NX * NY, LEVELS), jnp.float32).at[:, observed_column].add(gradient)
    field = field.reshape(shape)
    for sweep in range(SWEEPS):
        field = field + laplace(coeff * field)
    return vectors + jnp.dot(field.reshape(-1, LEVELS), vertical_factor, precision=HIGH).reshape(shape)
```

```python
import jax
import jax.numpy as jnp
from jax import lax
from jax.sharding import PartitionSpec as P

SWEEPS = 4

HIGH = lax.Precision.HIGH


def chain(axis, step):
    count = lax.axis_size(axis)
    return [(i, i + step) for i in range(count) if 0 <= i + step < count]


def with_halo(array, sides, width):
    for axis, dim in sides:
        length = array.shape[dim]
        last = lax.slice_in_dim(array, length - width, length, axis=dim)
        leading = lax.slice_in_dim(array, 0, width, axis=dim)
        low = lax.ppermute(last, axis, chain(axis, 1))
        high = lax.ppermute(leading, axis, chain(axis, -1))
        array = jnp.concatenate([low, array, high], axis=dim)
    return array


def fold_halo(array, sides, width):
    for axis, dim in sides:
        length = array.shape[dim]
        low = lax.slice_in_dim(array, 0, width, axis=dim)
        high = lax.slice_in_dim(array, length - width, length, axis=dim)
        array = lax.slice_in_dim(array, width, length - width, axis=dim)
        to_low = lax.ppermute(high, axis, chain(axis, 1))
        to_high = lax.ppermute(low, axis, chain(axis, -1))
        inner = array.shape[dim] - width
        pads = lambda before, after: [
            (before, after, 0) if d == dim else (0, 0, 0) for d in range(array.ndim)
        ]
        array = array + lax.pad(to_low, 0.0, pads(0, inner)) + lax.pad(to_high, 0.0, pads(inner, 0))
    return array


def diffusion_matrix(coeff, tile_x, tile_y):
    ext_x, ext_y = coeff.shape
    shape = (ext_x, ext_y, tile_x * tile_y)
    row = lax.broadcasted_iota(jnp.int32, shape, 0) - SWEEPS
    col = lax.broadcasted_iota(jnp.int32, shape, 1) - SWEEPS
    cell = lax.broadcasted_iota(jnp.int32, shape, 2)
    field = ((row == cell // tile_y) & (col == cell % tile_y)).astype(jnp.float32)
    for _ in range(SWEEPS):
        scaled = coeff[:, :, None] * field
        padded = jnp.pad(scaled, ((1, 1), (1, 1), (0, 0)))
        beside_all = (
            padded[2:, 1:-1] + padded[:-2, 1:-1] + padded[1:-1, 2:] + padded[1:-1, :-2]
        )
        field = field + beside_all - 4.0 * scaled
    return field.reshape(ext_x * ext_y, tile_x * tile_y)


def product(spec, a, b):
    return jnp.einsum(spec, a, b, precision=HIGH)


def body(
    vectors,
    diffusivity,
    vertical_factor,
    weight_first,
    bias_first,
    weight_second,
    bias_second,
    weight_out,
    error_inverse,
    observed_column,
    owner_count,
    observed_state,
    channel_mask,
):
    pairs, tile_x, tile_y, levels = vectors.shape
    count_x = lax.axis_size("gx")
    count_y = lax.axis_size("gy")
    devices = count_x * count_y
    slots = observed_column.shape[0]
    bucket = slots // devices
    grid_wide = tile_y * count_y
    cells = tile_x * tile_y
    position = jnp.arange(slots, dtype=jnp.int32)
    grid_row = observed_column // grid_wide
    grid_col = observed_column % grid_wide
    target_dev = grid_row // tile_x * count_y + grid_col // tile_y
    local_cell = grid_row % tile_x * tile_y + grid_col % tile_y
    in_use = position < owner_count[0]
    earlier = (
        (target_dev[:, None] == target_dev[None, :])
        & in_use[None, :]
        & (position[None, :] < position[:, None])
    )
    ordinal = jnp.sum(earlier.astype(jnp.int32), axis=1)
    target = jnp.where(in_use, target_dev * bucket + ordinal, slots)
    place = (position[:, None] == target[None, :]).astype(jnp.float32)
    labelled = jnp.concatenate(
        [observed_state, (local_cell + 1).astype(jnp.float32)[:, None]], axis=1
    )
    carried = lax.all_to_all(
        product("tn,nk->tk", place, labelled),
        ("gx", "gy"),
        split_axis=0,
        concat_axis=0,
        tiled=True,
    )
    asked = jnp.round(carried[:, levels]).astype(jnp.int32) - 1
    carried = carried[:, :levels]
    live = (asked >= 0).astype(jnp.float32)
    owner_mask = jnp.broadcast_to(
        channel_mask[:, None, :], (devices, bucket, channel_mask.shape[1])
    )
    gate = owner_mask.reshape(slots, -1).astype(jnp.float32) * live[:, None]
    pick = (asked[:, None] == jnp.arange(cells, dtype=jnp.int32)[None, :]).astype(jnp.float32)

    sides = (("gx", 0), ("gy", 1))
    spread = diffusion_matrix(with_halo(diffusivity, sides, SWEEPS), tile_x, tile_y)
    around = with_halo(vectors, (("gx", 1), ("gy", 2)), SWEEPS)
    lifted = product("lk,lh->kh", vertical_factor, weight_first)
    smooth = product("ec,vek->vck", spread, around.reshape(pairs, -1, levels))
    first = product("vck,kh->vch", smooth, lifted)

    hidden_one = jnp.tanh(product("nk,kh->nh", carried, weight_first) + bias_first)
    hidden_two = jnp.tanh(product("nh,hg->ng", hidden_one, weight_second) + bias_second)
    slope_one = 1.0 - hidden_one * hidden_one
    slope_two = 1.0 - hidden_two * hidden_two
    tangent = product("nc,vch->vnh", pick, first) * slope_one
    tangent = product("vnh,hg->vng", tangent, weight_second) * slope_two
    tangent = product("vng,gc->vnc", tangent, weight_out)
    weighted = gate * product("vnc,cd->vnd", gate * tangent, error_inverse)
    gradient = product("vnc,gc->vng", weighted, weight_out) * slope_two
    gradient = product("vng,hg->vnh", gradient, weight_second) * slope_one
    gradient = product("nc,vnh->vch", pick, gradient)
    gradient = product("vch,kh->vck", gradient, lifted)
    field = product("ec,vck->vek", spread, gradient)
    field = field.reshape(pairs, tile_x + 2 * SWEEPS, tile_y + 2 * SWEEPS, levels)
    return vectors + fold_halo(field, (("gy", 2), ("gx", 1)), SWEEPS)


def solution(mesh):
    in_specs = (
        P(None, "gx", "gy", None),
        P("gx", "gy"),
        P(),
        P(),
        P(),
        P(),
        P(),
        P(),
        P(),
        P(("gx", "gy")),
        P(("gx", "gy")),
        P(("gx", "gy"), None),
        P(),
    )
    out_specs = P(None, "gx", "gy", None)
    return jax.shard_map(body, mesh=mesh, in_specs=in_specs, out_specs=out_specs, check_vma=False)
```

```python
import functools

import jax
import jax.numpy as jnp
from jax import lax
from jax.experimental import pallas as pl
from jax.experimental.pallas import tpu as pltpu
from jax.sharding import PartitionSpec as P

SWEEPS = 4
LANES = 128
GRID_WIDE = 48
GRID_LEFT = 8
F32 = jnp.float32
BF16 = jnp.bfloat16
MESH = pl.DeviceIdType.MESH
ANY = pl.BlockSpec(memory_space=pl.ANY)
VMEM = pl.BlockSpec(memory_space=pltpu.VMEM)
SMEM = pl.BlockSpec(memory_space=pltpu.SMEM)


def split(x):
    high = x.astype(BF16)
    return high, (x - high.astype(F32)).astype(BF16)


def dot(a, b, transposed=False):
    dims = (((1,), (1 if transposed else 0,)), ((), ()))
    return lax.dot_general(a, b, dims, preferred_element_type=F32)


def dot3(a, b, transposed=False):
    (ah, al), (bh, bl) = a, b
    return dot(ah, bh, transposed) + (dot(ah, bl, transposed) + dot(al, bh, transposed))


def pieces(tile_x, tile_y):
    along, across, corner = SWEEPS * tile_y, SWEEPS * tile_x, SWEEPS * SWEEPS
    first, last, left, right = 0, along, 2 * along, 2 * along + across
    low = across - corner
    sends = (
        ((1, 0), last, along),
        ((-1, 0), first, along),
        ((0, 1), right, across),
        ((0, -1), left, across),
        ((1, 1), right + low, corner),
        ((1, -1), left + low, corner),
        ((-1, 1), right, corner),
        ((-1, -1), left, corner),
    )
    table, start = [], 0
    for step, source, size in sends:
        table.append((step, source, size, start))
        start += size
    return table, start


def pack_kernel(tile, count_ref, column_ref, row_ref, state_ref, vectors_ref, edge_coeff_ref, packed_ref, edges_ref):
    tile_x, tile_y, count_x, count_y = tile
    slots, levels = state_ref.shape
    devices = count_x * count_y
    wide = tile_y * count_y

    def device(column):
        return column // wide // tile_x * count_y + column % wide // tile_y

    columns = row_ref[...]
    target = device(columns)
    cell = columns // wide % tile_x * tile_y + columns % wide % tile_y
    shape = (slots, slots)
    mine = lax.broadcasted_iota(jnp.int32, shape, 1)
    other = lax.broadcasted_iota(jnp.int32, shape, 0)
    used = count_ref[0]
    earlier = (device(column_ref[...]) == target) & (other < used) & (other < mine)
    ordinal = jnp.sum(earlier.astype(F32), axis=0, keepdims=True).astype(jnp.int32)
    live = lax.broadcasted_iota(jnp.int32, (1, slots), 1) < used
    place = (other == jnp.where(live, ordinal * devices + target, slots)).astype(F32)
    label = jnp.sum(place * (cell + 1).astype(F32), axis=1, keepdims=True)
    place = place.astype(BF16)
    high, rest = split(state_ref[...])
    low = (state_ref[...] - high.astype(F32) - rest.astype(F32)).astype(BF16)
    moved = dot(place, high) + (dot(place, rest) + dot(place, low))
    tail = levels % LANES
    parts = -(-(levels + 1) // LANES)
    bucket = slots // devices
    for part in range(parts):
        if part < parts - 1:
            block = moved[:, part * LANES : (part + 1) * LANES]
        else:
            block = jnp.concatenate(
                [
                    moved[:, part * LANES :],
                    label,
                    jnp.zeros((slots, LANES - tail - 1), F32),
                ],
                axis=1,
            )
        for turn in range(bucket):
            packed_ref[pl.ds(turn * parts + part, devices, stride=bucket * parts), :] = block[
                turn * devices : (turn + 1) * devices
            ]

    along, across = SWEEPS * tile_y, SWEEPS * tile_x
    cells = tile_x * tile_y
    for v in range(vectors_ref.shape[0]):
        edges_ref[v, 0:along, 0:levels] = vectors_ref[v, 0:along, :]
        edges_ref[v, along : 2 * along, 0:levels] = vectors_ref[v, cells - along :, :]
        for i in range(tile_x):
            left = vectors_ref[v, i * tile_y : i * tile_y + SWEEPS, :]
            right = vectors_ref[v, (i + 1) * tile_y - SWEEPS : (i + 1) * tile_y, :]
            at = 2 * along + SWEEPS * i
            edges_ref[v, at : at + SWEEPS, 0:levels] = left
            edges_ref[v, at + across : at + across + SWEEPS, 0:levels] = right
        edges_ref[v, :, levels : levels + 1] = edge_coeff_ref[...]


def send_pieces(table, source_at, target_at, sends, receives, back):
    me_x, me_y = lax.axis_index("gx"), lax.axis_index("gy")
    count_x, count_y = lax.axis_size("gx"), lax.axis_size("gy")
    copies = []
    for k, (step, source, size, start) in enumerate(table):
        sign = -1 if back else 1
        peer = {
            "gx": lax.rem(me_x + sign * step[0] + count_x, count_x),
            "gy": lax.rem(me_y + sign * step[1] + count_y, count_y),
        }
        copy = pltpu.make_async_remote_copy(
            src_ref=source_at(source, start, size),
            dst_ref=target_at(source, start, size),
            send_sem=sends.at[k],
            recv_sem=receives.at[k],
            device_id=peer,
            device_id_type=MESH,
        )
        copy.start()
        copies.append(copy)
    return copies


def exchange_kernel(table, edges, packed, halo, carried, sends, receives, all_send, all_recv, own_sem):
    count_y = lax.axis_size("gy")
    devices = lax.axis_size("gx") * count_y
    me = lax.axis_index("gx") * count_y + lax.axis_index("gy")
    rows = lambda ref, start, size: ref.at[:, pl.ds(start, size), :]
    copies = send_pieces(
        table,
        lambda source, start, size: rows(edges, source, size),
        lambda source, start, size: rows(halo, start, size),
        sends,
        receives,
        False,
    )
    own = pltpu.make_async_copy(packed.at[me], carried.at[me], own_sem)
    own.start()

    def send(k, carry):
        peer = lax.rem(me + k, devices)
        pltpu.make_async_remote_copy(
            src_ref=packed.at[peer],
            dst_ref=carried.at[me],
            send_sem=all_send,
            recv_sem=all_recv,
            device_id={"gx": peer // count_y, "gy": lax.rem(peer, count_y)},
            device_id_type=MESH,
        ).start()
        return carry

    lax.fori_loop(1, devices, send, 0)
    own.wait()
    for copy in copies:
        copy.wait()
    others = pl.ds(0, devices - 1)
    every = pltpu.make_async_remote_copy(
        src_ref=packed.at[others],
        dst_ref=carried.at[others],
        send_sem=all_send,
        recv_sem=all_recv,
        device_id={"gx": lax.rem(lax.axis_index("gx") + 1, lax.axis_size("gx"))},
        device_id_type=MESH,
    )
    every.wait()


def return_kernel(table, outward, landed, sends, receives):
    rows = lambda ref, start, size: ref.at[:, pl.ds(start, size), :]
    copies = send_pieces(
        table,
        lambda source, start, size: rows(outward, start, size),
        lambda source, start, size: rows(landed, start, size),
        sends,
        receives,
        True,
    )
    for copy in copies:
        copy.wait()


def spread_rows(tile_x, tile_y):
    at = lambda i, j: (i + SWEEPS) * GRID_WIDE + GRID_LEFT + j
    blocks = [(at(i, 0), tile_y) for i in range(tile_x)]
    blocks += [(at(i - SWEEPS, 0), tile_y) for i in range(SWEEPS)]
    blocks += [(at(i + tile_x, 0), tile_y) for i in range(SWEEPS)]
    blocks += [(at(i, -SWEEPS), SWEEPS) for i in range(tile_x)]
    blocks += [(at(i, tile_y), SWEEPS) for i in range(tile_x)]
    for i0 in (-SWEEPS, tile_x):
        for j0 in (-SWEEPS, tile_y):
            blocks += [(at(i0 + i, j0), SWEEPS) for i in range(SWEEPS)]
    table, start = [], 0
    for source, size in blocks:
        table.append((source, start, size))
        start += size
    return table


def network_kernel(
    tile,
    vectors,
    halo,
    carried,
    coeff,
    mask,
    bias_first,
    bias_second,
    vertical_any,
    first_any,
    second_any,
    out_any,
    inverse_any,
    base,
    outward,
    vertical,
    first,
    second,
    out,
    inverse,
    grid_coeff,
    grid,
    spread,
    lifted,
    spread_high,
    spread_low,
    smooth_high,
    smooth_low,
    slope_one,
    slope_two,
    gate,
    sems,
):
    tile_x, tile_y, count_x, count_y = tile
    cells = tile_x * tile_y
    levels = vectors.shape[2]
    loads = []
    for k, (source, target) in enumerate(
        (
            (vertical_any, vertical),
            (first_any, first),
            (second_any, second),
            (out_any, out),
            (inverse_any, inverse),
        )
    ):
        load = pltpu.make_async_copy(source, target, sems.at[k])
        load.start()
        loads.append(load)

    order = spread_rows(tile_x, tile_y)
    grid_coeff[...] = jnp.zeros(grid_coeff.shape, F32)
    for source, start, size in order:
        if start < cells:
            column = coeff[start : start + size, :]
        else:
            column = halo[0, start - cells : start - cells + size, levels : levels + 1]
        grid_coeff[source : source + size, :] = jnp.broadcast_to(column, (size, LANES))
    chunk_x = LANES // tile_y
    near = (chunk_x + 2 * SWEEPS) * GRID_WIDE
    me_x, me_y = lax.axis_index("gx") * tile_x, lax.axis_index("gy") * tile_y
    grid[...] = jnp.zeros(grid.shape, F32)
    for q in range(tile_x // chunk_x):
        row = lax.broadcasted_iota(jnp.int32, (near, LANES), 0)
        lane = lax.broadcasted_iota(jnp.int32, (near, LANES), 1)
        i, j = row // GRID_WIDE - SWEEPS, row % GRID_WIDE - GRID_LEFT
        x, y = i + q * chunk_x + me_x, j + me_y
        inside = (x >= 0) & (x < tile_x * count_x) & (y >= 0) & (y < tile_y * count_y)
        begin = q * chunk_x * GRID_WIDE
        scale = jnp.where(inside, grid_coeff[begin : begin + near, :], 0.0)
        field = ((i == lane // tile_y) & (j == lane % tile_y)).astype(F32)
        for _ in range(SWEEPS):
            scaled = scale * field
            beside = (
                pltpu.roll(scaled, 1, 0)
                + pltpu.roll(scaled, near - 1, 0)
                + pltpu.roll(scaled, GRID_WIDE, 0)
                + pltpu.roll(scaled, near - GRID_WIDE, 0)
            )
            field = field + beside - 4.0 * scaled
        grid[begin : begin + near, q * LANES : (q + 1) * LANES] = jnp.where(inside, field, 0.0)
    for source, start, size in order:
        spread[start : start + size, :] = grid[source : source + size, :]
    total = order[-1][1] + order[-1][2]
    spread[total:, :] = jnp.zeros((spread.shape[0] - total, cells), F32)
    spread_high[...], spread_low[...] = split(spread[0:total, :])
    smooth_high[...], smooth_low[...] = split(jnp.transpose(spread[...]))

    loads[0].wait()
    loads[1].wait()
    first_split = split(first[...])
    lifted[...] = dot3(split(jnp.transpose(vertical[...])), first_split)

    devices = mask.shape[0]
    parts = -(-(levels + 1) // LANES)
    turns = carried.shape[0] // (devices * parts)
    tail = levels % LANES
    profile, label = [], []
    for turn in range(turns):
        blocks = [
            carried[pl.ds(turn * parts + part, devices, stride=turns * parts), :]
            for part in range(parts)
        ]
        label.append(blocks[-1][:, tail : tail + 1])
        profile.append(jnp.concatenate(blocks, axis=1)[:, 0:levels])
    profile = jnp.concatenate(profile, axis=0)
    slots = turns * devices
    gate_mask = mask[...].astype(F32)
    picks = []
    for turn in range(turns):
        live = (label[turn] > 0.5).astype(F32)
        gate[turn * devices : (turn + 1) * devices, :] = gate_mask * live
        across = jnp.transpose(jnp.broadcast_to(label[turn], (devices, LANES)))[0:1, :]
        picks.append(across)
    asked_row = jnp.concatenate(picks, axis=1)
    asked_column = jnp.concatenate(label, axis=0)
    number = lax.broadcasted_iota(jnp.int32, (slots, cells), 1).astype(F32) + 1.0
    pick = (jnp.abs(number - asked_column) < 0.5).astype(F32).astype(BF16)
    number = lax.broadcasted_iota(jnp.int32, (cells, slots), 0).astype(F32) + 1.0
    put = (jnp.abs(number - asked_row) < 0.5).astype(F32).astype(BF16)

    hidden = jnp.tanh(dot3(split(profile), first_split) + bias_first[...])
    slope_one[...] = 1.0 - hidden * hidden
    loads[2].wait()
    second_split = split(second[...])
    hidden = jnp.tanh(dot3(split(hidden), second_split) + bias_second[...])
    slope_two[...] = 1.0 - hidden * hidden
    loads[3].wait()
    loads[4].wait()

    def one_vector(v, carry):
        own = (smooth_high[:, 0:cells], smooth_low[:, 0:cells])
        around = (smooth_high[:, cells:total], smooth_low[:, cells:total])
        smooth = dot3(own, split(vectors[v])) + dot3(around, split(halo[v, :, 0:levels]))
        lifted_split = split(lifted[...])
        at_cells = dot3(split(smooth), lifted_split)
        high, low = split(at_cells)
        tangent = (dot(pick, high) + dot(pick, low)) * slope_one[...]
        weight = split(second[...])
        tangent = dot3(split(tangent), weight) * slope_two[...]
        weight = split(out[...])
        tangent = dot3(split(tangent), weight) * gate[...]
        weighted = dot3(split(tangent), split(inverse[...])) * gate[...]
        gradient = dot3(split(weighted), weight, True) * slope_two[...]
        weight = split(second[...])
        gradient = dot3(split(gradient), weight, True) * slope_one[...]
        high, low = split(gradient)
        gradient = dot(put, high) + dot(put, low)
        gradient = split(dot3(split(gradient), lifted_split, True))
        base[v] = vectors[v] + dot3((spread_high[0:cells, :], spread_low[0:cells, :]), gradient)
        outward[v] = dot3((spread_high[cells:total, :], spread_low[cells:total, :]), gradient)
        return carry

    lax.fori_loop(0, vectors.shape[0], one_vector, 0)


def finish_kernel(tile, base, landed, result):
    tile_x, tile_y, _, _ = tile
    cells = tile_x * tile_y
    along, across = SWEEPS * tile_y, SWEEPS * tile_x
    for v in range(base.shape[0]):
        result[v] = base[v]
        result[v, cells - along :, :] += landed[v, 0:along, :]
        result[v, 0:along, :] += landed[v, along : 2 * along, :]
        corners = 2 * along + 2 * across
        size = SWEEPS * SWEEPS
        for i in range(tile_x):
            start = 2 * along + SWEEPS * i
            right = landed[v, start : start + SWEEPS, :]
            left = landed[v, start + across : start + across + SWEEPS, :]
            if i < SWEEPS:
                at = corners + SWEEPS * i
                left += landed[v, at + 3 * size : at + 3 * size + SWEEPS, :]
                right += landed[v, at + 2 * size : at + 2 * size + SWEEPS, :]
            if i >= tile_x - SWEEPS:
                at = corners + SWEEPS * (i - tile_x + SWEEPS)
                left += landed[v, at + size : at + size + SWEEPS, :]
                right += landed[v, at : at + SWEEPS, :]
            result[v, i * tile_y : i * tile_y + SWEEPS, :] += left
            result[v, (i + 1) * tile_y - SWEEPS : (i + 1) * tile_y, :] += right


def shaped(*shape):
    return jax.ShapeDtypeStruct(shape, F32)


LIMIT = 60 * 1024 * 1024


def body(
    vectors,
    diffusivity,
    vertical_factor,
    weight_first,
    bias_first,
    weight_second,
    bias_second,
    weight_out,
    error_inverse,
    observed_column,
    owner_count,
    observed_state,
    channel_mask,
):
    pairs, tile_x, tile_y, levels = vectors.shape
    units, channels = weight_out.shape
    count_x = lax.axis_size("gx")
    count_y = lax.axis_size("gy")
    devices = count_x * count_y
    tile = (tile_x, tile_y, count_x, count_y)
    slots = observed_column.shape[0]
    bucket = slots // devices
    cells = tile_x * tile_y
    parts = -(-(levels + 1) // LANES)
    table, halo_rows = pieces(tile_x, tile_y)
    flat = vectors.reshape(pairs, cells, levels)
    coeff = diffusivity.reshape(cells, 1)
    edge_coeff = jnp.concatenate(
        [
            diffusivity[:SWEEPS].reshape(-1),
            diffusivity[-SWEEPS:].reshape(-1),
            diffusivity[:, :SWEEPS].reshape(-1),
            diffusivity[:, -SWEEPS:].reshape(-1),
        ]
    )[:, None]
    edge_rows = edge_coeff.shape[0]

    packed, edges = pl.pallas_call(
        functools.partial(pack_kernel, tile),
        out_shape=(shaped(slots * parts, LANES), shaped(pairs, edge_rows, levels + 1)),
        in_specs=[SMEM] + [VMEM] * 5,
        out_specs=(VMEM, VMEM),
        compiler_params=pltpu.CompilerParams(vmem_limit_bytes=LIMIT),
    )(owner_count, observed_column[:, None], observed_column[None, :], observed_state, flat, edge_coeff)

    dma = pltpu.SemaphoreType.DMA
    halo, carried = pl.pallas_call(
        functools.partial(exchange_kernel, table),
        out_shape=(
            shaped(pairs, halo_rows, levels + 1),
            shaped(devices, 1, bucket * parts * LANES),
        ),
        in_specs=[ANY, ANY],
        out_specs=(ANY, ANY),
        scratch_shapes=[dma((8,)), dma((8,)), dma, dma, dma],
        compiler_params=pltpu.CompilerParams(has_side_effects=True),
    )(edges, packed.reshape(devices, 1, bucket * parts * LANES))

    vm = pltpu.VMEM
    grid_rows = (tile_x + 2 * SWEEPS) * GRID_WIDE
    total = cells + halo_rows
    padded = -(-total // LANES) * LANES
    base, outward = pl.pallas_call(
        functools.partial(network_kernel, tile),
        out_shape=(shaped(pairs, cells, levels), shaped(pairs, halo_rows, levels)),
        in_specs=[VMEM] * 7 + [ANY] * 5,
        out_specs=(VMEM, VMEM),
        scratch_shapes=[
            vm((levels, levels), F32),
            vm((levels, units), F32),
            vm((units, units), F32),
            vm((units, channels), F32),
            vm((channels, channels), F32),
            vm((grid_rows, LANES), F32),
            vm((grid_rows, cells), F32),
            vm((padded, cells), F32),
            vm((levels, units), F32),
            vm((total, cells), BF16),
            vm((total, cells), BF16),
            vm((cells, padded), BF16),
            vm((cells, padded), BF16),
            vm((slots, units), F32),
            vm((slots, units), F32),
            vm((slots, channels), F32),
            dma((5,)),
        ],
        compiler_params=pltpu.CompilerParams(vmem_limit_bytes=LIMIT),
    )(
        flat,
        halo,
        carried.reshape(slots * parts, LANES),
        coeff,
        channel_mask,
        bias_first[None, :],
        bias_second[None, :],
        vertical_factor,
        weight_first,
        weight_second,
        weight_out,
        error_inverse,
    )

    landed = pl.pallas_call(
        functools.partial(return_kernel, table),
        out_shape=shaped(pairs, halo_rows, levels),
        in_specs=[ANY],
        out_specs=ANY,
        scratch_shapes=[dma((8,)), dma((8,))],
        compiler_params=pltpu.CompilerParams(has_side_effects=True),
    )(outward)

    result = pl.pallas_call(
        functools.partial(finish_kernel, tile),
        out_shape=shaped(pairs, cells, levels),
        in_specs=[VMEM, VMEM],
        out_specs=VMEM,
        compiler_params=pltpu.CompilerParams(vmem_limit_bytes=LIMIT),
    )(base, landed)
    return result.reshape(vectors.shape)


def solution(mesh):
    in_specs = (
        P(None, "gx", "gy", None),
        P("gx", "gy"),
        P(),
        P(),
        P(),
        P(),
        P(),
        P(),
        P(),
        P(("gx", "gy")),
        P(("gx", "gy")),
        P(("gx", "gy"), None),
        P(),
    )
    out_specs = P(None, "gx", "gy", None)
    return jax.shard_map(body, mesh=mesh, in_specs=in_specs, out_specs=out_specs, check_vma=False)
```

```python
import functools

import jax
import jax.numpy as jnp
from jax import lax
from jax.experimental import pallas as pl
from jax.experimental.pallas import tpu as pltpu
from jax.sharding import PartitionSpec as P

SWEEPS = 4
LANES = 128
GRID_WIDE = 48
GRID_LEFT = 8
F32 = jnp.float32
BF16 = jnp.bfloat16
MESH = pl.DeviceIdType.MESH
ANY = pl.BlockSpec(memory_space=pl.ANY)
VMEM = pl.BlockSpec(memory_space=pltpu.VMEM)
SMEM = pl.BlockSpec(memory_space=pltpu.SMEM)


def split(x):
    high = x.astype(BF16)
    return high, (x - high.astype(F32)).astype(BF16)


def dot(a, b, transposed=False):
    dims = (((1,), (1 if transposed else 0,)), ((), ()))
    return lax.dot_general(a, b, dims, preferred_element_type=F32)


def dot3(a, b, transposed=False):
    (ah, al), (bh, bl) = a, b
    return dot(ah, bh, transposed) + (dot(ah, bl, transposed) + dot(al, bh, transposed))


def pieces(tile_x, tile_y):
    along, across, corner = SWEEPS * tile_y, SWEEPS * tile_x, SWEEPS * SWEEPS
    first, last, left, right = 0, along, 2 * along, 2 * along + across
    low = across - corner
    sends = (
        ((1, 0), last, along),
        ((-1, 0), first, along),
        ((0, 1), right, across),
        ((0, -1), left, across),
        ((1, 1), right + low, corner),
        ((1, -1), left + low, corner),
        ((-1, 1), right, corner),
        ((-1, -1), left, corner),
    )
    table, start = [], 0
    for step, source, size in sends:
        table.append((step, source, size, start))
        start += size
    return table, start


def cell_columns(diffusivity_ref, square_ref):
    tile_x, tile_y = diffusivity_ref.shape
    square_ref[...] = jnp.zeros((LANES, LANES), F32)
    square_ref[0:tile_x, 0:tile_y] = diffusivity_ref[...]
    return jnp.transpose(square_ref[...])


def pack_kernel(tile, count_ref, row_ref, state_ref, vectors_ref, diffusivity_ref, packed_ref, edges_ref, square_ref):
    tile_x, tile_y, count_x, count_y = tile
    levels, slots = state_ref.shape
    devices = count_x * count_y
    wide = tile_y * count_y
    columns = row_ref[...]
    target = columns // wide // tile_x * count_y + columns % wide // tile_y
    cell = columns // wide % tile_x * tile_y + columns % wide % tile_y
    shape = (slots, slots)
    mine = lax.broadcasted_iota(jnp.int32, shape, 1)
    other = lax.broadcasted_iota(jnp.int32, shape, 0)
    used = count_ref[0]
    other_target = jnp.transpose(jnp.broadcast_to(target.astype(F32), (LANES, slots)))[:, 0:1]
    same = jnp.abs(other_target - target.astype(F32)) < 0.5
    earlier = same & (other < used) & (other < mine)
    ordinal = jnp.sum(earlier.astype(F32), axis=0, keepdims=True).astype(jnp.int32)
    live = lax.broadcasted_iota(jnp.int32, (1, slots), 1) < used
    place = (other == jnp.where(live, ordinal * devices + target, slots)).astype(F32)
    label = jnp.sum(place * (cell + 1).astype(F32), axis=1, keepdims=True)
    place = place.astype(BF16)
    high, rest = split(state_ref[...])
    low = (state_ref[...] - high.astype(F32) - rest.astype(F32)).astype(BF16)
    moved = dot(place, high, True) + (dot(place, rest, True) + dot(place, low, True))
    tail = levels % LANES
    parts = -(-(levels + 1) // LANES)
    bucket = slots // devices
    for part in range(parts):
        if part < parts - 1:
            block = moved[:, part * LANES : (part + 1) * LANES]
        else:
            block = jnp.concatenate(
                [
                    moved[:, part * LANES :],
                    label,
                    jnp.zeros((slots, LANES - tail - 1), F32),
                ],
                axis=1,
            )
        for turn in range(bucket):
            packed_ref[:, turn * parts + part, :] = block[turn * devices : (turn + 1) * devices]

    along, across = SWEEPS * tile_y, SWEEPS * tile_x
    cells = tile_x * tile_y
    latitude = cell_columns(diffusivity_ref, square_ref)
    for v in range(vectors_ref.shape[0]):
        edges_ref[v, 0:along, 0:levels] = vectors_ref[v, 0:along, :]
        edges_ref[v, along : 2 * along, 0:levels] = vectors_ref[v, cells - along :, :]
        for i in range(SWEEPS):
            at, last = i * tile_y, tile_x - SWEEPS + i
            edges_ref[v, at : at + tile_y, levels : levels + 1] = latitude[0:tile_y, i : i + 1]
            edges_ref[v, along + at : along + at + tile_y, levels : levels + 1] = latitude[
                0:tile_y, last : last + 1
            ]
        for i in range(tile_x):
            left = vectors_ref[v, i * tile_y : i * tile_y + SWEEPS, :]
            right = vectors_ref[v, (i + 1) * tile_y - SWEEPS : (i + 1) * tile_y, :]
            at = 2 * along + SWEEPS * i
            edges_ref[v, at : at + SWEEPS, 0:levels] = left
            edges_ref[v, at + across : at + across + SWEEPS, 0:levels] = right
            edges_ref[v, at : at + SWEEPS, levels : levels + 1] = latitude[0:SWEEPS, i : i + 1]
            edges_ref[v, at + across : at + across + SWEEPS, levels : levels + 1] = latitude[
                tile_y - SWEEPS : tile_y, i : i + 1
            ]


def piece_copies(table, source_at, target_at, sends, receives, back):
    me_x, me_y = lax.axis_index("gx"), lax.axis_index("gy")
    count_x, count_y = lax.axis_size("gx"), lax.axis_size("gy")
    sign = -1 if back else 1
    copies = []
    for k, (step, source, size, start) in enumerate(table):
        peer = {
            "gx": lax.rem(me_x + sign * step[0] + count_x, count_x),
            "gy": lax.rem(me_y + sign * step[1] + count_y, count_y),
        }
        copies.append(
            pltpu.make_async_remote_copy(
                src_ref=source_at(source, start, size),
                dst_ref=target_at(source, start, size),
                send_sem=sends.at[k],
                recv_sem=receives.at[k],
                device_id=peer,
                device_id_type=MESH,
            )
        )
    return copies


def return_copies(table, outward, landed, sends, receives, v):
    rows = lambda ref, start, size: ref.at[v, pl.ds(start, size), :]
    return piece_copies(
        table,
        lambda source, start, size: rows(outward, start, size),
        lambda source, start, size: rows(landed, start, size),
        sends.at[v],
        receives.at[v],
        True,
    )


def bucket_copy(packed, carried, source, target, send_sem, recv_sem, peer):
    count_y = lax.axis_size("gy")
    return pltpu.make_async_remote_copy(
        src_ref=packed.at[source],
        dst_ref=carried.at[target],
        send_sem=send_sem,
        recv_sem=recv_sem,
        device_id={"gx": peer // count_y, "gy": lax.rem(peer, count_y)},
        device_id_type=MESH,
    )


def spread_rows(tile_x, tile_y):
    at = lambda i, j: (i + SWEEPS) * GRID_WIDE + GRID_LEFT + j
    blocks = [(at(i, 0), tile_y) for i in range(tile_x)]
    blocks += [(at(i - SWEEPS, 0), tile_y) for i in range(SWEEPS)]
    blocks += [(at(i + tile_x, 0), tile_y) for i in range(SWEEPS)]
    blocks += [(at(i, -SWEEPS), SWEEPS) for i in range(tile_x)]
    blocks += [(at(i, tile_y), SWEEPS) for i in range(tile_x)]
    for i0 in (-SWEEPS, tile_x):
        for j0 in (-SWEEPS, tile_y):
            blocks += [(at(i0 + i, j0), SWEEPS) for i in range(SWEEPS)]
    table, start = [], 0
    for source, size in blocks:
        table.append((source, start, size))
        start += size
    return table


def network_kernel(
    tile,
    table,
    edges,
    packed,
    vectors,
    diffusivity,
    mask,
    biases,
    vertical_any,
    first_any,
    second_any,
    out_any,
    inverse_any,
    result,
    halo,
    carried,
    outward,
    landed,
    at_cells,
    square,
    vertical,
    first,
    second,
    out,
    inverse,
    grid_coeff,
    grid,
    spread,
    lifted,
    spread_high,
    spread_low,
    smooth_high,
    smooth_low,
    slope_one,
    slope_two,
    gate,
    sems,
    halo_send,
    halo_recv,
    back_send,
    back_recv,
    all_send,
    all_recv,
    own_sem,
):
    tile_x, tile_y, count_x, count_y = tile
    cells = tile_x * tile_y
    levels = vectors.shape[2]
    pairs = vectors.shape[0]
    devices = count_x * count_y
    me = lax.axis_index("gx") * count_y + lax.axis_index("gy")
    rows = lambda ref, start, size: ref.at[:, pl.ds(start, size), :]
    halo_copies = piece_copies(
        table,
        lambda source, start, size: rows(edges, source, size),
        lambda source, start, size: rows(halo, start, size),
        halo_send,
        halo_recv,
        False,
    )
    for copy in halo_copies:
        copy.start()
    own_copy = pltpu.make_async_copy(packed.at[me], carried.at[me], own_sem)
    own_copy.start()

    def send(k, carry):
        peer = lax.rem(me + k, devices)
        bucket_copy(packed, carried, peer, me, all_send, all_recv, peer).start()
        return carry

    lax.fori_loop(1, devices, send, 0)
    loads = []
    for k, (source, target) in enumerate(
        (
            (vertical_any, vertical),
            (first_any, first),
            (second_any, second),
            (out_any, out),
            (inverse_any, inverse),
        )
    ):
        load = pltpu.make_async_copy(source, target, sems.at[k])
        load.start()
        loads.append(load)

    loads[0].wait()
    loads[1].wait()
    first_split = split(first[...])
    lifted[...] = dot3(split(jnp.transpose(vertical[...])), first_split)

    for copy in halo_copies:
        copy.wait()
    latitude = cell_columns(diffusivity, square)
    order = spread_rows(tile_x, tile_y)
    grid_coeff[...] = jnp.zeros(grid_coeff.shape, F32)
    for source, start, size in order:
        if start < cells:
            column = latitude[0:tile_y, start // tile_y : start // tile_y + 1]
        else:
            column = halo[0, start - cells : start - cells + size, levels : levels + 1]
        grid_coeff[source : source + size, :] = jnp.broadcast_to(column, (size, LANES))
    chunk_x = LANES // tile_y
    near = (chunk_x + 2 * SWEEPS) * GRID_WIDE
    me_x, me_y = lax.axis_index("gx") * tile_x, lax.axis_index("gy") * tile_y
    grid[...] = jnp.zeros(grid.shape, F32)
    for q in range(tile_x // chunk_x):
        row = lax.broadcasted_iota(jnp.int32, (near, LANES), 0)
        lane = lax.broadcasted_iota(jnp.int32, (near, LANES), 1)
        i, j = row // GRID_WIDE - SWEEPS, row % GRID_WIDE - GRID_LEFT
        x, y = i + q * chunk_x + me_x, j + me_y
        inside = (x >= 0) & (x < tile_x * count_x) & (y >= 0) & (y < tile_y * count_y)
        begin = q * chunk_x * GRID_WIDE
        scale = jnp.where(inside, grid_coeff[begin : begin + near, :], 0.0)
        field = ((i == lane // tile_y) & (j == lane % tile_y)).astype(F32)
        for _ in range(SWEEPS):
            scaled = scale * field
            beside = (
                pltpu.roll(scaled, 1, 0)
                + pltpu.roll(scaled, near - 1, 0)
                + pltpu.roll(scaled, GRID_WIDE, 0)
                + pltpu.roll(scaled, near - GRID_WIDE, 0)
            )
            field = field + beside - 4.0 * scaled
        grid[begin : begin + near, q * LANES : (q + 1) * LANES] = jnp.where(inside, field, 0.0)
    for source, start, size in order:
        spread[start : start + size, :] = grid[source : source + size, :]
    total = order[-1][1] + order[-1][2]
    spread[total:, :] = jnp.zeros((spread.shape[0] - total, cells), F32)
    spread_high[...], spread_low[...] = split(spread[0:total, :])
    smooth_high[...], smooth_low[...] = split(jnp.transpose(spread[...]))

    def before(v, carry):
        own = (smooth_high[:, 0:cells], smooth_low[:, 0:cells])
        around = (smooth_high[:, cells:total], smooth_low[:, cells:total])
        smooth = dot3(own, split(vectors[v])) + dot3(around, split(halo[v, :, 0:levels]))
        at_cells[v] = dot3(split(smooth), split(lifted[...]))
        return carry

    lax.fori_loop(0, pairs, before, 0)
    own_copy.wait()
    others = pl.ds(0, devices - 1)
    bucket_copy(packed, carried, others, others, all_send, all_recv, lax.rem(me + 1, devices)).wait()

    parts = -(-(levels + 1) // LANES)
    turns = carried.shape[1] // parts
    tail = levels % LANES
    profile, label = [], []
    for turn in range(turns):
        blocks = [
            carried[:, turn * parts + part, :]
            for part in range(parts)
        ]
        label.append(blocks[-1][:, tail : tail + 1])
        profile.append(jnp.concatenate(blocks, axis=1)[:, 0:levels])
    profile = jnp.concatenate(profile, axis=0)
    slots = turns * devices
    gate_mask = jnp.transpose(mask[...].astype(F32))
    picks = []
    for turn in range(turns):
        live = (label[turn] > 0.5).astype(F32)
        gate[turn * devices : (turn + 1) * devices, :] = gate_mask * live
        across = jnp.transpose(jnp.broadcast_to(label[turn], (devices, LANES)))[0:1, :]
        picks.append(across)
    asked_row = jnp.concatenate(picks, axis=1)
    asked_column = jnp.concatenate(label, axis=0)
    number = lax.broadcasted_iota(jnp.int32, (slots, cells), 1).astype(F32) + 1.0
    pick = (jnp.abs(number - asked_column) < 0.5).astype(F32).astype(BF16)
    number = lax.broadcasted_iota(jnp.int32, (cells, slots), 0).astype(F32) + 1.0
    put = (jnp.abs(number - asked_row) < 0.5).astype(F32).astype(BF16)

    hidden = jnp.tanh(dot3(split(profile), first_split) + biases[0:1, :])
    slope_one[...] = 1.0 - hidden * hidden
    loads[2].wait()
    second_split = split(second[...])
    hidden = jnp.tanh(dot3(split(hidden), second_split) + biases[1:2, :])
    slope_two[...] = 1.0 - hidden * hidden
    loads[3].wait()
    loads[4].wait()

    def one_vector(v, carry):
        lifted_split = split(lifted[...])
        high, low = split(at_cells[v])
        tangent = (dot(pick, high) + dot(pick, low)) * slope_one[...]
        weight = split(second[...])
        tangent = dot3(split(tangent), weight) * slope_two[...]
        weight = split(out[...])
        tangent = dot3(split(tangent), weight, True) * gate[...]
        weighted = dot3(split(tangent), split(inverse[...])) * gate[...]
        gradient = dot3(split(weighted), weight) * slope_two[...]
        weight = split(second[...])
        gradient = dot3(split(gradient), weight, True) * slope_one[...]
        high, low = split(gradient)
        gradient = dot(put, high) + dot(put, low)
        gradient = split(dot3(split(gradient), lifted_split, True))
        outward[v] = dot3((spread_high[cells:total, :], spread_low[cells:total, :]), gradient)
        result[v] = vectors[v] + dot3((spread_high[0:cells, :], spread_low[0:cells, :]), gradient)
        for copy in return_copies(table, outward, landed, back_send, back_recv, v):
            copy.start()
        return carry

    lax.fori_loop(0, pairs, one_vector, 0)

    def finish(v, carry):
        for copy in return_copies(table, outward, landed, back_send, back_recv, v):
            copy.wait()
        add_landed(tile, v, landed, result)
        return carry

    lax.fori_loop(0, pairs, finish, 0)


def add_landed(tile, v, landed, result):
    tile_x, tile_y, _, _ = tile
    cells = tile_x * tile_y
    along, across = SWEEPS * tile_y, SWEEPS * tile_x
    result[v, cells - along :, :] += landed[v, 0:along, :]
    result[v, 0:along, :] += landed[v, along : 2 * along, :]
    corners = 2 * along + 2 * across
    size = SWEEPS * SWEEPS
    for i in range(tile_x):
        start = 2 * along + SWEEPS * i
        right = landed[v, start : start + SWEEPS, :]
        left = landed[v, start + across : start + across + SWEEPS, :]
        if i < SWEEPS:
            at = corners + SWEEPS * i
            left += landed[v, at + 3 * size : at + 3 * size + SWEEPS, :]
            right += landed[v, at + 2 * size : at + 2 * size + SWEEPS, :]
        if i >= tile_x - SWEEPS:
            at = corners + SWEEPS * (i - tile_x + SWEEPS)
            left += landed[v, at + size : at + size + SWEEPS, :]
            right += landed[v, at : at + SWEEPS, :]
        result[v, i * tile_y : i * tile_y + SWEEPS, :] += left
        result[v, (i + 1) * tile_y - SWEEPS : (i + 1) * tile_y, :] += right


def shaped(*shape):
    return jax.ShapeDtypeStruct(shape, F32)


LIMIT = 60 * 1024 * 1024


def body(
    vectors,
    diffusivity,
    vertical_factor,
    weight_first,
    bias_first,
    weight_second,
    bias_second,
    weight_out,
    error_inverse,
    observed_column,
    owner_count,
    observed_state,
    channel_mask,
):
    pairs, tile_x, tile_y, levels = vectors.shape
    units, channels = weight_out.shape
    count_x = lax.axis_size("gx")
    count_y = lax.axis_size("gy")
    devices = count_x * count_y
    tile = (tile_x, tile_y, count_x, count_y)
    slots = observed_column.shape[0]
    bucket = slots // devices
    cells = tile_x * tile_y
    parts = -(-(levels + 1) // LANES)
    table, halo_rows = pieces(tile_x, tile_y)
    flat = vectors.reshape(pairs, cells, levels)
    edge_rows = 2 * SWEEPS * (tile_x + tile_y)
    dma, vm = pltpu.SemaphoreType.DMA, pltpu.VMEM

    packed, edges = pl.pallas_call(
        functools.partial(pack_kernel, tile),
        out_shape=(shaped(devices, bucket * parts, LANES), shaped(pairs, edge_rows, levels + 1)),
        in_specs=[SMEM] + [VMEM] * 4,
        out_specs=(VMEM, VMEM),
        scratch_shapes=[vm((LANES, LANES), F32)],
        compiler_params=pltpu.CompilerParams(vmem_limit_bytes=LIMIT),
    )(owner_count, observed_column[None, :], observed_state.T, flat, diffusivity)

    grid_rows = (tile_x + 2 * SWEEPS) * GRID_WIDE
    total = cells + halo_rows
    padded = -(-total // LANES) * LANES
    result = pl.pallas_call(
        functools.partial(network_kernel, tile, table),
        out_shape=shaped(pairs, cells, levels),
        in_specs=[ANY] * 2 + [VMEM] * 4 + [ANY] * 5,
        out_specs=VMEM,
        scratch_shapes=[
            vm((pairs, halo_rows, levels + 1), F32),
            vm((devices, bucket * parts, LANES), F32),
            vm((pairs, halo_rows, levels), F32),
            vm((pairs, halo_rows, levels), F32),
            vm((pairs, cells, units), F32),
            vm((LANES, LANES), F32),
            vm((levels, levels), F32),
            vm((levels, units), F32),
            vm((units, units), F32),
            vm((channels, units), F32),
            vm((channels, channels), F32),
            vm((grid_rows, LANES), F32),
            vm((grid_rows, cells), F32),
            vm((padded, cells), F32),
            vm((levels, units), F32),
            vm((total, cells), BF16),
            vm((total, cells), BF16),
            vm((cells, padded), BF16),
            vm((cells, padded), BF16),
            vm((slots, units), F32),
            vm((slots, units), F32),
            vm((slots, channels), F32),
            dma((5,)),
            dma((8,)),
            dma((8,)),
            dma((pairs, 8)),
            dma((pairs, 8)),
            dma,
            dma,
            dma,
        ],
        compiler_params=pltpu.CompilerParams(vmem_limit_bytes=LIMIT, has_side_effects=True),
    )(
        edges,
        packed,
        flat,
        diffusivity,
        channel_mask.T,
        jnp.stack([bias_first, bias_second]),
        vertical_factor,
        weight_first,
        weight_second,
        weight_out.T,
        error_inverse,
    )
    return result.reshape(vectors.shape)


def solution(mesh):
    in_specs = (
        P(None, "gx", "gy", None),
        P("gx", "gy"),
        P(),
        P(),
        P(),
        P(),
        P(),
        P(),
        P(),
        P(("gx", "gy")),
        P(("gx", "gy")),
        P(("gx", "gy"), None),
        P(),
    )
    out_specs = P(None, "gx", "gy", None)
    return jax.shard_map(body, mesh=mesh, in_specs=in_specs, out_specs=out_specs, check_vma=False)
```

```python
import functools

import jax
import jax.numpy as jnp
from jax import lax
from jax.experimental import pallas as pl
from jax.experimental.pallas import tpu as pltpu
from jax.sharding import PartitionSpec as P

SWEEPS = 4
LANES = 128
GRID_WIDE = 48
GRID_LEFT = 8
F32 = jnp.float32
BF16 = jnp.bfloat16
MESH = pl.DeviceIdType.MESH
ANY = pl.BlockSpec(memory_space=pl.ANY)
VMEM = pl.BlockSpec(memory_space=pltpu.VMEM)
SMEM = pl.BlockSpec(memory_space=pltpu.SMEM)


def split(x):
    high = x.astype(BF16)
    return high, (x - high.astype(F32)).astype(BF16)


def dot(a, b, transposed=False):
    dims = (((1,), (1 if transposed else 0,)), ((), ()))
    return lax.dot_general(a, b, dims, preferred_element_type=F32)


def dot3(a, b, transposed=False):
    (ah, al), (bh, bl) = a, b
    return dot(ah, bh, transposed) + (dot(ah, bl, transposed) + dot(al, bh, transposed))


def pieces(tile_x, tile_y):
    along, across, corner = SWEEPS * tile_y, SWEEPS * tile_x, SWEEPS * SWEEPS
    first, last, left, right = 0, tile_x * tile_y - along, 0, across
    low = across - corner
    sends = (
        ((1, 0), last, along),
        ((-1, 0), first, along),
        ((0, 1), right, across),
        ((0, -1), left, across),
        ((1, 1), right + low, corner),
        ((1, -1), left + low, corner),
        ((-1, 1), right, corner),
        ((-1, -1), left, corner),
    )
    table, start = [], 0
    for step, source, size in sends:
        table.append((step, source, size, start))
        start += size
    return table, start


def pack_edges(tile, vectors, edges):
    tile_x, tile_y, _, _ = tile
    across = SWEEPS * tile_x
    for v in range(vectors.shape[0]):
        for i in range(tile_x):
            at = SWEEPS * i
            edges[v, at : at + SWEEPS, :] = vectors[v, i * tile_y : i * tile_y + SWEEPS, :]
            edges[v, across + at : across + at + SWEEPS, :] = vectors[
                v, (i + 1) * tile_y - SWEEPS : (i + 1) * tile_y, :
            ]


def pack_profiles(tile, used, columns, state, packed):
    tile_x, tile_y, count_x, count_y = tile
    levels, slots = state.shape
    devices = count_x * count_y
    wide = tile_y * count_y
    target = columns // wide // tile_x * count_y + columns % wide // tile_y
    cell = columns // wide % tile_x * tile_y + columns % wide % tile_y
    shape = (slots, slots)
    mine = lax.broadcasted_iota(jnp.int32, shape, 1)
    other = lax.broadcasted_iota(jnp.int32, shape, 0)
    other_target = jnp.transpose(jnp.broadcast_to(target.astype(F32), (LANES, slots)))[:, 0:1]
    same = jnp.abs(other_target - target.astype(F32)) < 0.5
    earlier = same & (other < used) & (other < mine)
    ordinal = jnp.sum(earlier.astype(F32), axis=0, keepdims=True).astype(jnp.int32)
    live = lax.broadcasted_iota(jnp.int32, (1, slots), 1) < used
    place = (other == jnp.where(live, ordinal * devices + target, slots)).astype(F32)
    label = jnp.sum(place * (cell + 1).astype(F32), axis=1, keepdims=True)
    place = place.astype(BF16)
    high, rest = split(state)
    low = (state - high.astype(F32) - rest.astype(F32)).astype(BF16)
    moved = dot(place, high, True) + (dot(place, rest, True) + dot(place, low, True))
    tail = levels % LANES
    parts = -(-(levels + 1) // LANES)
    bucket = slots // devices
    for part in range(parts):
        if part < parts - 1:
            block = moved[:, part * LANES : (part + 1) * LANES]
        else:
            block = jnp.concatenate(
                [
                    moved[:, part * LANES :],
                    label,
                    jnp.zeros((slots, LANES - tail - 1), F32),
                ],
                axis=1,
            )
        for turn in range(bucket):
            packed[:, turn * parts + part, :] = block[turn * devices : (turn + 1) * devices]


def piece_copies(table, source_at, target_at, sends, receives, back):
    me_x, me_y = lax.axis_index("gx"), lax.axis_index("gy")
    count_x, count_y = lax.axis_size("gx"), lax.axis_size("gy")
    sign = -1 if back else 1
    copies = []
    for k, (step, source, size, start) in enumerate(table):
        peer = {
            "gx": lax.rem(me_x + sign * step[0] + count_x, count_x),
            "gy": lax.rem(me_y + sign * step[1] + count_y, count_y),
        }
        copies.append(
            pltpu.make_async_remote_copy(
                src_ref=source_at(source, start, size),
                dst_ref=target_at(source, start, size),
                send_sem=sends.at[k],
                recv_sem=receives.at[k],
                device_id=peer,
                device_id_type=MESH,
            )
        )
    return copies


def return_copies(table, outward, landed, sends, receives, v):
    rows = lambda ref, start, size: ref.at[v, pl.ds(start, size), :]
    return piece_copies(
        table,
        lambda source, start, size: rows(outward, start, size),
        lambda source, start, size: rows(landed, start, size),
        sends.at[v],
        receives.at[v],
        True,
    )


def bucket_copy(packed, carried, source, target, send_sem, recv_sem, peer):
    count_y = lax.axis_size("gy")
    return pltpu.make_async_remote_copy(
        src_ref=packed.at[source],
        dst_ref=carried.at[target],
        send_sem=send_sem,
        recv_sem=recv_sem,
        device_id={"gx": peer // count_y, "gy": lax.rem(peer, count_y)},
        device_id_type=MESH,
    )


def spread_rows(tile_x, tile_y):
    at = lambda i, j: (i + SWEEPS) * GRID_WIDE + GRID_LEFT + j
    low_x, low_y = tile_x - SWEEPS, tile_y - SWEEPS
    blocks = [(at(i, 0), tile_y, 8, 0, i) for i in range(tile_x)]
    blocks += [(at(i - SWEEPS, 0), tile_y, 0, 0, low_x + i) for i in range(SWEEPS)]
    blocks += [(at(i + tile_x, 0), tile_y, 1, 0, i) for i in range(SWEEPS)]
    blocks += [(at(i, -SWEEPS), SWEEPS, 2, low_y, i) for i in range(tile_x)]
    blocks += [(at(i, tile_y), SWEEPS, 3, 0, i) for i in range(tile_x)]
    slot = 4
    for i0, from_x in ((-SWEEPS, low_x), (tile_x, 0)):
        for j0, from_y in ((-SWEEPS, low_y), (tile_y, 0)):
            blocks += [(at(i0 + i, j0), SWEEPS, slot, from_y, from_x + i) for i in range(SWEEPS)]
            slot += 1
    table, start = [], 0
    for source, size, slot, from_y, from_x in blocks:
        table.append((source, start, size, slot, from_y, from_x))
        start += size
    return table


def network_kernel(
    tile,
    table,
    count,
    columns,
    state,
    flat,
    diffusivity,
    mask,
    biases,
    vertical_any,
    first_any,
    second_any,
    out_any,
    inverse_any,
    result,
    vectors,
    edges,
    packed,
    coeffs,
    halo,
    carried,
    outward,
    landed,
    at_cells,
    square,
    vertical,
    first,
    second,
    out,
    inverse,
    grid_coeff,
    grid,
    spread,
    lifted,
    spread_high,
    spread_low,
    smooth_high,
    smooth_low,
    slope_one,
    slope_two,
    gate,
    sems,
    tile_sems,
    coeff_send,
    coeff_recv,
    halo_send,
    halo_recv,
    back_send,
    back_recv,
    all_send,
    all_recv,
    own_sem,
):
    tile_x, tile_y, count_x, count_y = tile
    cells = tile_x * tile_y
    levels = vectors.shape[2]
    pairs = vectors.shape[0]
    devices = count_x * count_y
    me = lax.axis_index("gx") * count_y + lax.axis_index("gy")
    rows = lambda ref, start, size: ref.at[:, pl.ds(start, size), :]

    def halo_copies(part, array):
        return piece_copies(
            table[part],
            lambda source, start, size: rows(array, source, size),
            lambda source, start, size: rows(halo, start, size),
            halo_send.at[part],
            halo_recv.at[part],
            False,
        )

    coeff_copies = []
    for k, entry in enumerate(table):
        coeff_copies += piece_copies(
            [entry],
            lambda source, start, size: diffusivity,
            lambda source, start, size, k=k: coeffs.at[k],
            coeff_send.at[k : k + 1],
            coeff_recv.at[k : k + 1],
            False,
        )
    far_copies = halo_copies(slice(0, 2), flat)
    for copy in coeff_copies + far_copies:
        copy.start()
    own_coeff = pltpu.make_async_copy(diffusivity, coeffs.at[8], tile_sems.at[0])
    own_coeff.start()
    own_tile = pltpu.make_async_copy(flat, vectors, tile_sems.at[1])
    own_tile.start()

    def send(k, carry):
        peer = lax.rem(me + k, devices)
        bucket_copy(packed, carried, peer, me, all_send, all_recv, peer).start()
        return carry

    loads = []
    for k, (source, target) in enumerate(
        (
            (vertical_any, vertical),
            (first_any, first),
            (second_any, second),
            (out_any, out),
            (inverse_any, inverse),
        )
    ):
        load = pltpu.make_async_copy(source, target, sems.at[k])
        load.start()
        loads.append(load)

    own_tile.wait()
    pack_edges(tile, vectors, edges)
    pack_profiles(tile, count[0], columns[...], state[...], packed)
    near_copies = halo_copies(slice(2, 8), edges)
    for copy in near_copies:
        copy.start()
    loads[0].wait()
    loads[1].wait()
    first_split = split(first[...])
    lifted[...] = dot3(split(jnp.transpose(vertical[...])), first_split)

    own_copy = pltpu.make_async_copy(packed.at[me], carried.at[me], own_sem)
    own_copy.start()
    lax.fori_loop(1, devices, send, 0)
    own_coeff.wait()
    for copy in coeff_copies:
        copy.wait()
    order = spread_rows(tile_x, tile_y)
    square[...] = jnp.zeros((LANES, LANES), F32)
    latitude = []
    for slot in range(9):
        square[0:tile_x, 0:tile_y] = coeffs[slot]
        latitude.append(jnp.transpose(square[...]))
    grid_coeff[...] = jnp.zeros(grid_coeff.shape, F32)
    for source, start, size, slot, from_y, from_x in order:
        column = latitude[slot][from_y : from_y + size, from_x : from_x + 1]
        grid_coeff[source : source + size, :] = jnp.broadcast_to(column, (size, LANES))
    chunk_x = LANES // tile_y
    near = (chunk_x + 2 * SWEEPS) * GRID_WIDE
    me_x, me_y = lax.axis_index("gx") * tile_x, lax.axis_index("gy") * tile_y
    grid[...] = jnp.zeros(grid.shape, F32)
    for q in range(tile_x // chunk_x):
        row = lax.broadcasted_iota(jnp.int32, (near, LANES), 0)
        lane = lax.broadcasted_iota(jnp.int32, (near, LANES), 1)
        i, j = row // GRID_WIDE - SWEEPS, row % GRID_WIDE - GRID_LEFT
        x, y = i + q * chunk_x + me_x, j + me_y
        inside = (x >= 0) & (x < tile_x * count_x) & (y >= 0) & (y < tile_y * count_y)
        begin = q * chunk_x * GRID_WIDE
        scale = jnp.where(inside, grid_coeff[begin : begin + near, :], 0.0)
        field = ((i == lane // tile_y) & (j == lane % tile_y)).astype(F32)
        for _ in range(SWEEPS):
            scaled = scale * field
            beside = (
                pltpu.roll(scaled, 1, 0)
                + pltpu.roll(scaled, near - 1, 0)
                + pltpu.roll(scaled, GRID_WIDE, 0)
                + pltpu.roll(scaled, near - GRID_WIDE, 0)
            )
            field = field + beside - 4.0 * scaled
        grid[begin : begin + near, q * LANES : (q + 1) * LANES] = jnp.where(inside, field, 0.0)
    for source, start, size, _, _, _ in order:
        spread[start : start + size, :] = grid[source : source + size, :]
    total = order[-1][1] + order[-1][2]
    spread[total:, :] = jnp.zeros((spread.shape[0] - total, cells), F32)
    spread_high[...], spread_low[...] = split(spread[0:total, :])
    smooth_high[...], smooth_low[...] = split(jnp.transpose(spread[...]))

    for copy in far_copies + near_copies:
        copy.wait()

    def before(v, carry):
        own = (smooth_high[:, 0:cells], smooth_low[:, 0:cells])
        around = (smooth_high[:, cells:total], smooth_low[:, cells:total])
        smooth = dot3(own, split(vectors[v])) + dot3(around, split(halo[v, :, 0:levels]))
        at_cells[v] = dot3(split(smooth), split(lifted[...]))
        return carry

    lax.fori_loop(0, pairs, before, 0)
    own_copy.wait()
    others = pl.ds(0, devices - 1)
    bucket_copy(packed, carried, others, others, all_send, all_recv, lax.rem(me + 1, devices)).wait()

    parts = -(-(levels + 1) // LANES)
    turns = carried.shape[1] // parts
    tail = levels % LANES
    profile, label = [], []
    for turn in range(turns):
        blocks = [
            carried[:, turn * parts + part, :]
            for part in range(parts)
        ]
        label.append(blocks[-1][:, tail : tail + 1])
        profile.append(jnp.concatenate(blocks, axis=1)[:, 0:levels])
    profile = jnp.concatenate(profile, axis=0)
    slots = turns * devices
    gate_mask = jnp.transpose(mask[...].astype(F32))
    picks = []
    for turn in range(turns):
        live = (label[turn] > 0.5).astype(F32)
        gate[turn * devices : (turn + 1) * devices, :] = gate_mask * live
        across = jnp.transpose(jnp.broadcast_to(label[turn], (devices, LANES)))[0:1, :]
        picks.append(across)
    asked_row = jnp.concatenate(picks, axis=1)
    asked_column = jnp.concatenate(label, axis=0)
    number = lax.broadcasted_iota(jnp.int32, (slots, cells), 1).astype(F32) + 1.0
    pick = (jnp.abs(number - asked_column) < 0.5).astype(F32).astype(BF16)
    number = lax.broadcasted_iota(jnp.int32, (cells, slots), 0).astype(F32) + 1.0
    put = (jnp.abs(number - asked_row) < 0.5).astype(F32).astype(BF16)

    hidden = jnp.tanh(dot3(split(profile), first_split) + biases[0:1, :])
    slope_one[...] = 1.0 - hidden * hidden
    loads[2].wait()
    second_split = split(second[...])
    hidden = jnp.tanh(dot3(split(hidden), second_split) + biases[1:2, :])
    slope_two[...] = 1.0 - hidden * hidden
    loads[3].wait()
    loads[4].wait()

    def one_vector(v, carry):
        lifted_split = split(lifted[...])
        high, low = split(at_cells[v])
        tangent = (dot(pick, high) + dot(pick, low)) * slope_one[...]
        weight = split(second[...])
        tangent = dot3(split(tangent), weight) * slope_two[...]
        weight = split(out[...])
        tangent = dot3(split(tangent), weight, True) * gate[...]
        weighted = dot3(split(tangent), split(inverse[...])) * gate[...]
        gradient = dot3(split(weighted), weight) * slope_two[...]
        weight = split(second[...])
        gradient = dot3(split(gradient), weight, True) * slope_one[...]
        high, low = split(gradient)
        gradient = dot(put, high) + dot(put, low)
        gradient = split(dot3(split(gradient), lifted_split, True))
        outward[v] = dot3((spread_high[cells:total, :], spread_low[cells:total, :]), gradient)
        result[v] = vectors[v] + dot3((spread_high[0:cells, :], spread_low[0:cells, :]), gradient)
        for copy in return_copies(table, outward, landed, back_send, back_recv, v):
            copy.start()
        return carry

    lax.fori_loop(0, pairs, one_vector, 0)

    def finish(v, carry):
        for copy in return_copies(table, outward, landed, back_send, back_recv, v):
            copy.wait()
        add_landed(tile, v, landed, result)
        return carry

    lax.fori_loop(0, pairs, finish, 0)


def add_landed(tile, v, landed, result):
    tile_x, tile_y, _, _ = tile
    cells = tile_x * tile_y
    along, across = SWEEPS * tile_y, SWEEPS * tile_x
    result[v, cells - along :, :] += landed[v, 0:along, :]
    result[v, 0:along, :] += landed[v, along : 2 * along, :]
    corners = 2 * along + 2 * across
    size = SWEEPS * SWEEPS
    for i in range(tile_x):
        start = 2 * along + SWEEPS * i
        right = landed[v, start : start + SWEEPS, :]
        left = landed[v, start + across : start + across + SWEEPS, :]
        if i < SWEEPS:
            at = corners + SWEEPS * i
            left += landed[v, at + 3 * size : at + 3 * size + SWEEPS, :]
            right += landed[v, at + 2 * size : at + 2 * size + SWEEPS, :]
        if i >= tile_x - SWEEPS:
            at = corners + SWEEPS * (i - tile_x + SWEEPS)
            left += landed[v, at + size : at + size + SWEEPS, :]
            right += landed[v, at : at + SWEEPS, :]
        result[v, i * tile_y : i * tile_y + SWEEPS, :] += left
        result[v, (i + 1) * tile_y - SWEEPS : (i + 1) * tile_y, :] += right


def shaped(*shape):
    return jax.ShapeDtypeStruct(shape, F32)


LIMIT = 60 * 1024 * 1024


def body(
    vectors,
    diffusivity,
    vertical_factor,
    weight_first,
    bias_first,
    weight_second,
    bias_second,
    weight_out,
    error_inverse,
    observed_column,
    owner_count,
    observed_state,
    channel_mask,
):
    pairs, tile_x, tile_y, levels = vectors.shape
    units, channels = weight_out.shape
    count_x = lax.axis_size("gx")
    count_y = lax.axis_size("gy")
    devices = count_x * count_y
    tile = (tile_x, tile_y, count_x, count_y)
    slots = observed_column.shape[0]
    bucket = slots // devices
    cells = tile_x * tile_y
    parts = -(-(levels + 1) // LANES)
    table, halo_rows = pieces(tile_x, tile_y)
    flat = vectors.reshape(pairs, cells, levels)
    dma, vm = pltpu.SemaphoreType.DMA, pltpu.VMEM
    grid_rows = (tile_x + 2 * SWEEPS) * GRID_WIDE
    total = cells + halo_rows
    padded = -(-total // LANES) * LANES
    result = pl.pallas_call(
        functools.partial(network_kernel, tile, table),
        out_shape=shaped(pairs, cells, levels),
        in_specs=[SMEM] + [VMEM] * 2 + [ANY] * 2 + [VMEM] * 2 + [ANY] * 5,
        out_specs=VMEM,
        scratch_shapes=[
            vm((pairs, cells, levels), F32),
            vm((pairs, 2 * SWEEPS * tile_x, levels), F32),
            vm((devices, bucket * parts, LANES), F32),
            vm((9, tile_x, tile_y), F32),
            vm((pairs, halo_rows, levels), F32),
            vm((devices, bucket * parts, LANES), F32),
            vm((pairs, halo_rows, levels), F32),
            vm((pairs, halo_rows, levels), F32),
            vm((pairs, cells, units), F32),
            vm((LANES, LANES), F32),
            vm((levels, levels), F32),
            vm((levels, units), F32),
            vm((units, units), F32),
            vm((channels, units), F32),
            vm((channels, channels), F32),
            vm((grid_rows, LANES), F32),
            vm((grid_rows, cells), F32),
            vm((padded, cells), F32),
            vm((levels, units), F32),
            vm((total, cells), BF16),
            vm((total, cells), BF16),
            vm((cells, padded), BF16),
            vm((cells, padded), BF16),
            vm((slots, units), F32),
            vm((slots, units), F32),
            vm((slots, channels), F32),
            dma((5,)),
            dma((2,)),
            dma((8,)),
            dma((8,)),
            dma((8,)),
            dma((8,)),
            dma((pairs, 8)),
            dma((pairs, 8)),
            dma,
            dma,
            dma,
        ],
        compiler_params=pltpu.CompilerParams(vmem_limit_bytes=LIMIT, has_side_effects=True),
    )(
        owner_count,
        observed_column[None, :],
        observed_state.T,
        flat,
        diffusivity,
        channel_mask.T,
        jnp.stack([bias_first, bias_second]),
        vertical_factor,
        weight_first,
        weight_second,
        weight_out.T,
        error_inverse,
    )
    return result.reshape(vectors.shape)


def solution(mesh):
    in_specs = (
        P(None, "gx", "gy", None),
        P("gx", "gy"),
        P(),
        P(),
        P(),
        P(),
        P(),
        P(),
        P(),
        P(("gx", "gy")),
        P(("gx", "gy")),
        P(("gx", "gy"), None),
        P(),
    )
    out_specs = P(None, "gx", "gy", None)
    return jax.shard_map(body, mesh=mesh, in_specs=in_specs, out_specs=out_specs, check_vma=False)
```

```python
import functools

import jax
import jax.numpy as jnp
from jax import lax
from jax.experimental import pallas as pl
from jax.experimental.pallas import tpu as pltpu
from jax.sharding import PartitionSpec as P

SWEEPS = 4
LANES = 128
GRID_WIDE = 48
GRID_LEFT = 8
F32 = jnp.float32
BF16 = jnp.bfloat16
MESH = pl.DeviceIdType.MESH
ANY = pl.BlockSpec(memory_space=pl.ANY)
VMEM = pl.BlockSpec(memory_space=pltpu.VMEM)
SMEM = pl.BlockSpec(memory_space=pltpu.SMEM)


def split(x):
    high = x.astype(BF16)
    return high, (x - high.astype(F32)).astype(BF16)


def dot(a, b, transposed=False):
    dims = (((1,), (1 if transposed else 0,)), ((), ()))
    return lax.dot_general(a, b, dims, preferred_element_type=F32)


def dot3(a, b, transposed=False):
    (ah, al), (bh, bl) = a, b
    return dot(ah, bh, transposed) + (dot(ah, bl, transposed) + dot(al, bh, transposed))


def pieces(tile_x, tile_y):
    along, across, corner = SWEEPS * tile_y, SWEEPS * tile_x, SWEEPS * SWEEPS
    first, last, left, right = 0, tile_x * tile_y - along, 0, across
    low = across - corner
    sends = (
        ((1, 0), last, along),
        ((-1, 0), first, along),
        ((0, 1), right, across),
        ((0, -1), left, across),
        ((1, 1), right + low, corner),
        ((1, -1), left + low, corner),
        ((-1, 1), right, corner),
        ((-1, -1), left, corner),
    )
    table, start = [], 0
    for step, source, size in sends:
        table.append((step, source, size, start))
        start += size
    return table, start


def pack_edges(tile, vectors, edges):
    tile_x, tile_y, _, _ = tile
    across = SWEEPS * tile_x
    for v in range(vectors.shape[0]):
        for i in range(tile_x):
            at = SWEEPS * i
            edges[v, at : at + SWEEPS, :] = vectors[v, i * tile_y : i * tile_y + SWEEPS, :]
            edges[v, across + at : across + at + SWEEPS, :] = vectors[
                v, (i + 1) * tile_y - SWEEPS : (i + 1) * tile_y, :
            ]


def pack_profiles(tile, used, columns, state, packed):
    tile_x, tile_y, count_x, count_y = tile
    levels, slots = state.shape
    devices = count_x * count_y
    wide = tile_y * count_y
    target = columns // wide // tile_x * count_y + columns % wide // tile_y
    cell = columns // wide % tile_x * tile_y + columns % wide % tile_y
    shape = (slots, slots)
    mine = lax.broadcasted_iota(jnp.int32, shape, 1)
    other = lax.broadcasted_iota(jnp.int32, shape, 0)
    other_target = jnp.transpose(jnp.broadcast_to(target.astype(F32), (LANES, slots)))[:, 0:1]
    same = jnp.abs(other_target - target.astype(F32)) < 0.5
    earlier = same & (other < used) & (other < mine)
    ordinal = jnp.sum(earlier.astype(F32), axis=0, keepdims=True).astype(jnp.int32)
    live = lax.broadcasted_iota(jnp.int32, (1, slots), 1) < used
    place = (other == jnp.where(live, ordinal * devices + target, slots)).astype(F32)
    label = jnp.sum(place * (cell + 1).astype(F32), axis=1, keepdims=True)
    place = place.astype(BF16)
    high, rest = split(state)
    low = (state - high.astype(F32) - rest.astype(F32)).astype(BF16)
    moved = dot(place, high, True) + (dot(place, rest, True) + dot(place, low, True))
    tail = levels % LANES
    parts = -(-(levels + 1) // LANES)
    bucket = slots // devices
    for part in range(parts):
        if part < parts - 1:
            block = moved[:, part * LANES : (part + 1) * LANES]
        else:
            block = jnp.concatenate(
                [
                    moved[:, part * LANES :],
                    label,
                    jnp.zeros((slots, LANES - tail - 1), F32),
                ],
                axis=1,
            )
        for turn in range(bucket):
            packed[:, turn * parts + part, :] = block[turn * devices : (turn + 1) * devices]


def piece_copies(table, source_at, target_at, sends, receives, back):
    me_x, me_y = lax.axis_index("gx"), lax.axis_index("gy")
    count_x, count_y = lax.axis_size("gx"), lax.axis_size("gy")
    sign = -1 if back else 1
    copies = []
    for k, (step, source, size, start) in enumerate(table):
        peer = {
            "gx": lax.rem(me_x + sign * step[0] + count_x, count_x),
            "gy": lax.rem(me_y + sign * step[1] + count_y, count_y),
        }
        copies.append(
            pltpu.make_async_remote_copy(
                src_ref=source_at(source, start, size),
                dst_ref=target_at(source, start, size),
                send_sem=sends.at[k],
                recv_sem=receives.at[k],
                device_id=peer,
                device_id_type=MESH,
            )
        )
    return copies


def return_copies(table, outward, landed, sends, receives, v):
    rows = lambda ref, start, size: ref.at[v, pl.ds(start, size), :]
    return piece_copies(
        table,
        lambda source, start, size: rows(outward, start, size),
        lambda source, start, size: rows(landed, start, size),
        sends.at[v],
        receives.at[v],
        True,
    )


def bucket_copy(packed, carried, source, target, send_sem, recv_sem, peer):
    count_y = lax.axis_size("gy")
    return pltpu.make_async_remote_copy(
        src_ref=packed.at[source],
        dst_ref=carried.at[target],
        send_sem=send_sem,
        recv_sem=recv_sem,
        device_id={"gx": peer // count_y, "gy": lax.rem(peer, count_y)},
        device_id_type=MESH,
    )


def one_row(ref):
    return jnp.concatenate([ref[i : i + 1, :] for i in range(ref.shape[0])], axis=1)


def spread_rows(tile_x, tile_y):
    at = lambda i, j: (i + SWEEPS) * GRID_WIDE + GRID_LEFT + j
    low_x, low_y = tile_x - SWEEPS, tile_y - SWEEPS
    blocks = [(at(i, 0), tile_y, 8, 0, i) for i in range(tile_x)]
    blocks += [(at(i - SWEEPS, 0), tile_y, 0, 0, low_x + i) for i in range(SWEEPS)]
    blocks += [(at(i + tile_x, 0), tile_y, 1, 0, i) for i in range(SWEEPS)]
    blocks += [(at(i, -SWEEPS), SWEEPS, 2, low_y, i) for i in range(tile_x)]
    blocks += [(at(i, tile_y), SWEEPS, 3, 0, i) for i in range(tile_x)]
    slot = 4
    for i0, from_x in ((-SWEEPS, low_x), (tile_x, 0)):
        for j0, from_y in ((-SWEEPS, low_y), (tile_y, 0)):
            blocks += [(at(i0 + i, j0), SWEEPS, slot, from_y, from_x + i) for i in range(SWEEPS)]
            slot += 1
    table, start = [], 0
    for source, size, slot, from_y, from_x in blocks:
        table.append((source, start, size, slot, from_y, from_x))
        start += size
    return table


def network_kernel(
    tile,
    table,
    count,
    columns,
    state,
    flat,
    diffusivity,
    mask,
    bias_first,
    bias_second,
    vertical_any,
    first_any,
    second_any,
    out_any,
    inverse_any,
    result,
    vectors,
    edges,
    packed,
    coeffs,
    halo,
    carried,
    outward,
    landed,
    at_cells,
    square,
    vertical,
    first,
    second,
    out,
    inverse,
    grid_coeff,
    grid,
    spread,
    lifted,
    spread_high,
    spread_low,
    smooth_high,
    smooth_low,
    slope_one,
    slope_two,
    gate,
    sems,
    tile_sems,
    coeff_send,
    coeff_recv,
    halo_send,
    halo_recv,
    back_send,
    back_recv,
    all_send,
    all_recv,
    own_sem,
):
    tile_x, tile_y, count_x, count_y = tile
    cells = tile_x * tile_y
    levels = vectors.shape[2]
    pairs = vectors.shape[0]
    devices = count_x * count_y
    me = lax.axis_index("gx") * count_y + lax.axis_index("gy")
    rows = lambda ref, start, size: ref.at[:, pl.ds(start, size), :]

    def halo_copies(part, array):
        return piece_copies(
            table[part],
            lambda source, start, size: rows(array, source, size),
            lambda source, start, size: rows(halo, start, size),
            halo_send.at[part],
            halo_recv.at[part],
            False,
        )

    coeff_copies = []
    for k, entry in enumerate(table):
        coeff_copies += piece_copies(
            [entry],
            lambda source, start, size: diffusivity,
            lambda source, start, size, k=k: coeffs.at[k],
            coeff_send.at[k : k + 1],
            coeff_recv.at[k : k + 1],
            False,
        )
    far_copies = halo_copies(slice(0, 2), flat)
    for copy in coeff_copies + far_copies:
        copy.start()
    own_coeff = pltpu.make_async_copy(diffusivity, coeffs.at[8], tile_sems.at[0])
    own_coeff.start()
    own_tile = pltpu.make_async_copy(flat, vectors, tile_sems.at[1])
    own_tile.start()

    def send(k, carry):
        peer = lax.rem(me + k, devices)
        bucket_copy(packed, carried, peer, me, all_send, all_recv, peer).start()
        return carry

    loads = []
    for k, (source, target) in enumerate(
        (
            (vertical_any, vertical),
            (first_any, first),
            (second_any, second),
            (out_any, out),
            (inverse_any, inverse),
        )
    ):
        load = pltpu.make_async_copy(source, target, sems.at[k])
        load.start()
        loads.append(load)

    own_tile.wait()
    pack_edges(tile, vectors, edges)
    pack_profiles(tile, count[0], columns[...], state[...], packed)
    near_copies = halo_copies(slice(2, 8), edges)
    for copy in near_copies:
        copy.start()
    loads[0].wait()
    loads[1].wait()
    first_split = split(first[...])
    lifted[...] = dot3(split(jnp.transpose(vertical[...])), first_split)

    own_copy = pltpu.make_async_copy(packed.at[me], carried.at[me], own_sem)
    own_copy.start()
    lax.fori_loop(1, devices, send, 0)
    own_coeff.wait()
    for copy in coeff_copies:
        copy.wait()
    order = spread_rows(tile_x, tile_y)
    square[...] = jnp.zeros((LANES, LANES), F32)
    latitude = []
    for slot in range(9):
        square[0:tile_x, 0:tile_y] = coeffs[slot]
        latitude.append(jnp.transpose(square[...]))
    grid_coeff[...] = jnp.zeros(grid_coeff.shape, F32)
    for source, start, size, slot, from_y, from_x in order:
        column = latitude[slot][from_y : from_y + size, from_x : from_x + 1]
        grid_coeff[source : source + size, :] = jnp.broadcast_to(column, (size, LANES))
    chunk_x = LANES // tile_y
    near = (chunk_x + 2 * SWEEPS) * GRID_WIDE
    me_x, me_y = lax.axis_index("gx") * tile_x, lax.axis_index("gy") * tile_y
    grid[...] = jnp.zeros(grid.shape, F32)
    for q in range(tile_x // chunk_x):
        row = lax.broadcasted_iota(jnp.int32, (near, LANES), 0)
        lane = lax.broadcasted_iota(jnp.int32, (near, LANES), 1)
        i, j = row // GRID_WIDE - SWEEPS, row % GRID_WIDE - GRID_LEFT
        x, y = i + q * chunk_x + me_x, j + me_y
        inside = (x >= 0) & (x < tile_x * count_x) & (y >= 0) & (y < tile_y * count_y)
        begin = q * chunk_x * GRID_WIDE
        scale = jnp.where(inside, grid_coeff[begin : begin + near, :], 0.0)
        field = ((i == lane // tile_y) & (j == lane % tile_y)).astype(F32)
        for _ in range(SWEEPS):
            scaled = scale * field
            beside = (
                pltpu.roll(scaled, 1, 0)
                + pltpu.roll(scaled, near - 1, 0)
                + pltpu.roll(scaled, GRID_WIDE, 0)
                + pltpu.roll(scaled, near - GRID_WIDE, 0)
            )
            field = field + beside - 4.0 * scaled
        grid[begin : begin + near, q * LANES : (q + 1) * LANES] = jnp.where(inside, field, 0.0)
    for source, start, size, _, _, _ in order:
        spread[start : start + size, :] = grid[source : source + size, :]
    total = order[-1][1] + order[-1][2]
    spread[total:, :] = jnp.zeros((spread.shape[0] - total, cells), F32)
    spread_high[...], spread_low[...] = split(spread[0:total, :])
    smooth_high[...], smooth_low[...] = split(jnp.transpose(spread[...]))

    for copy in far_copies + near_copies:
        copy.wait()

    def before(v, carry):
        own = (smooth_high[:, 0:cells], smooth_low[:, 0:cells])
        around = (smooth_high[:, cells:total], smooth_low[:, cells:total])
        smooth = dot3(own, split(vectors[v])) + dot3(around, split(halo[v, :, 0:levels]))
        at_cells[v] = dot3(split(smooth), split(lifted[...]))
        return carry

    lax.fori_loop(0, pairs, before, 0)
    own_copy.wait()
    others = pl.ds(0, devices - 1)
    bucket_copy(packed, carried, others, others, all_send, all_recv, lax.rem(me + 1, devices)).wait()

    parts = -(-(levels + 1) // LANES)
    turns = carried.shape[1] // parts
    tail = levels % LANES
    profile, label = [], []
    for turn in range(turns):
        blocks = [
            carried[:, turn * parts + part, :]
            for part in range(parts)
        ]
        label.append(blocks[-1][:, tail : tail + 1])
        profile.append(jnp.concatenate(blocks, axis=1)[:, 0:levels])
    profile = jnp.concatenate(profile, axis=0)
    slots = turns * devices
    gate_mask = jnp.transpose(mask[...].astype(F32))
    picks = []
    for turn in range(turns):
        live = (label[turn] > 0.5).astype(F32)
        gate[turn * devices : (turn + 1) * devices, :] = gate_mask * live
        across = jnp.transpose(jnp.broadcast_to(label[turn], (devices, LANES)))[0:1, :]
        picks.append(across)
    asked_row = jnp.concatenate(picks, axis=1)
    asked_column = jnp.concatenate(label, axis=0)
    number = lax.broadcasted_iota(jnp.int32, (slots, cells), 1).astype(F32) + 1.0
    pick = (jnp.abs(number - asked_column) < 0.5).astype(F32).astype(BF16)
    number = lax.broadcasted_iota(jnp.int32, (cells, slots), 0).astype(F32) + 1.0
    put = (jnp.abs(number - asked_row) < 0.5).astype(F32).astype(BF16)

    hidden = jnp.tanh(dot3(split(profile), first_split) + one_row(bias_first))
    slope_one[...] = 1.0 - hidden * hidden
    loads[2].wait()
    second_split = split(second[...])
    hidden = jnp.tanh(dot3(split(hidden), second_split) + one_row(bias_second))
    slope_two[...] = 1.0 - hidden * hidden
    loads[3].wait()
    loads[4].wait()

    def one_vector(v, carry):
        lifted_split = split(lifted[...])
        high, low = split(at_cells[v])
        tangent = (dot(pick, high) + dot(pick, low)) * slope_one[...]
        weight = split(second[...])
        tangent = dot3(split(tangent), weight) * slope_two[...]
        weight = split(out[...])
        tangent = dot3(split(tangent), weight, True) * gate[...]
        weighted = dot3(split(tangent), split(inverse[...])) * gate[...]
        gradient = dot3(split(weighted), weight) * slope_two[...]
        weight = split(second[...])
        gradient = dot3(split(gradient), weight, True) * slope_one[...]
        high, low = split(gradient)
        gradient = dot(put, high) + dot(put, low)
        gradient = split(dot3(split(gradient), lifted_split, True))
        outward[v] = dot3((spread_high[cells:total, :], spread_low[cells:total, :]), gradient)
        result[v] = vectors[v] + dot3((spread_high[0:cells, :], spread_low[0:cells, :]), gradient)
        for copy in return_copies(table, outward, landed, back_send, back_recv, v):
            copy.start()
        return carry

    lax.fori_loop(0, pairs, one_vector, 0)

    def finish(v, carry):
        for copy in return_copies(table, outward, landed, back_send, back_recv, v):
            copy.wait()
        add_landed(tile, v, landed, result)
        return carry

    lax.fori_loop(0, pairs, finish, 0)


def add_landed(tile, v, landed, result):
    tile_x, tile_y, _, _ = tile
    cells = tile_x * tile_y
    along, across = SWEEPS * tile_y, SWEEPS * tile_x
    result[v, cells - along :, :] += landed[v, 0:along, :]
    result[v, 0:along, :] += landed[v, along : 2 * along, :]
    corners = 2 * along + 2 * across
    size = SWEEPS * SWEEPS
    for i in range(tile_x):
        start = 2 * along + SWEEPS * i
        right = landed[v, start : start + SWEEPS, :]
        left = landed[v, start + across : start + across + SWEEPS, :]
        if i < SWEEPS:
            at = corners + SWEEPS * i
            left += landed[v, at + 3 * size : at + 3 * size + SWEEPS, :]
            right += landed[v, at + 2 * size : at + 2 * size + SWEEPS, :]
        if i >= tile_x - SWEEPS:
            at = corners + SWEEPS * (i - tile_x + SWEEPS)
            left += landed[v, at + size : at + size + SWEEPS, :]
            right += landed[v, at : at + SWEEPS, :]
        result[v, i * tile_y : i * tile_y + SWEEPS, :] += left
        result[v, (i + 1) * tile_y - SWEEPS : (i + 1) * tile_y, :] += right


def shaped(*shape):
    return jax.ShapeDtypeStruct(shape, F32)


LIMIT = 60 * 1024 * 1024


def body(
    vectors,
    diffusivity,
    vertical_factor,
    weight_first,
    bias_first,
    weight_second,
    bias_second,
    weight_out,
    error_inverse,
    observed_column,
    owner_count,
    observed_state,
    channel_mask,
):
    pairs, tile_x, tile_y, levels = vectors.shape
    units, channels = weight_out.shape
    count_x = lax.axis_size("gx")
    count_y = lax.axis_size("gy")
    devices = count_x * count_y
    tile = (tile_x, tile_y, count_x, count_y)
    slots = observed_column.shape[0]
    bucket = slots // devices
    cells = tile_x * tile_y
    parts = -(-(levels + 1) // LANES)
    table, halo_rows = pieces(tile_x, tile_y)
    flat = vectors.reshape(pairs, cells, levels)
    dma, vm = pltpu.SemaphoreType.DMA, pltpu.VMEM
    grid_rows = (tile_x + 2 * SWEEPS) * GRID_WIDE
    total = cells + halo_rows
    padded = -(-total // LANES) * LANES
    result = pl.pallas_call(
        functools.partial(network_kernel, tile, table),
        out_shape=shaped(pairs, cells, levels),
        in_specs=[SMEM] + [VMEM] * 2 + [ANY] * 2 + [VMEM] * 3 + [ANY] * 5,
        out_specs=VMEM,
        scratch_shapes=[
            vm((pairs, cells, levels), F32),
            vm((pairs, 2 * SWEEPS * tile_x, levels), F32),
            vm((devices, bucket * parts, LANES), F32),
            vm((9, tile_x, tile_y), F32),
            vm((pairs, halo_rows, levels), F32),
            vm((devices, bucket * parts, LANES), F32),
            vm((pairs, halo_rows, levels), F32),
            vm((pairs, halo_rows, levels), F32),
            vm((pairs, cells, units), F32),
            vm((LANES, LANES), F32),
            vm((levels, levels), F32),
            vm((levels, units), F32),
            vm((units, units), F32),
            vm((channels, units), F32),
            vm((channels, channels), F32),
            vm((grid_rows, LANES), F32),
            vm((grid_rows, cells), F32),
            vm((padded, cells), F32),
            vm((levels, units), F32),
            vm((total, cells), BF16),
            vm((total, cells), BF16),
            vm((cells, padded), BF16),
            vm((cells, padded), BF16),
            vm((slots, units), F32),
            vm((slots, units), F32),
            vm((slots, channels), F32),
            dma((5,)),
            dma((2,)),
            dma((8,)),
            dma((8,)),
            dma((8,)),
            dma((8,)),
            dma((pairs, 8)),
            dma((pairs, 8)),
            dma,
            dma,
            dma,
        ],
        compiler_params=pltpu.CompilerParams(vmem_limit_bytes=LIMIT, has_side_effects=True),
    )(
        owner_count,
        observed_column[None, :],
        observed_state.T,
        flat,
        diffusivity,
        channel_mask.T,
        bias_first.reshape(-1, LANES),
        bias_second.reshape(-1, LANES),
        vertical_factor,
        weight_first,
        weight_second,
        weight_out.T,
        error_inverse,
    )
    return result.reshape(vectors.shape)


def solution(mesh):
    in_specs = (
        P(None, "gx", "gy", None),
        P("gx", "gy"),
        P(),
        P(),
        P(),
        P(),
        P(),
        P(),
        P(),
        P(("gx", "gy")),
        P(("gx", "gy")),
        P(("gx", "gy"), None),
        P(),
    )
    out_specs = P(None, "gx", "gy", None)
    return jax.shard_map(body, mesh=mesh, in_specs=in_specs, out_specs=out_specs, check_vma=False)
```
